32 devices in a mesh: obs: 8 (over z, y), rep: 4 (over x, core).
Axes of the slice: x: 2, y: 2, z: 4, core: 2. Of those that a mesh axis runs over, the one named last changes fastest.
Arguments:
- jacobians: float32 [18, 131072], P(None, ('obs', 'rep')), may hold values from -3 to 3
- residuals: float32 [2, 131072], P(None, ('obs', 'rep')), may hold values from -6 to 6
- camera_local: int32 [131072], P(('obs', 'rep')), may hold values from 0 to 1023
- bucket_counts: int32 [32, 8], P(('obs', 'rep')), may hold values from 1 to 512, as said below
- camera_map: int32 [8192], replicated, may hold values from 0 to 8191, each once
Outputs:
- gradient: float32 [9, 8192], replicated
- camera_blocks: float32 [81, 8192], P(None, 'obs')
The draws below stay inside these ranges and needn't reach their ends.
Inputs may be any that keep to these rules, and one draw needn't show every extreme that they name: bucket_counts[s, d] counts the leading live slots of bucket d of source block s; exactly one destination d has all 512 slots live from every source block, and every other bucket has at most 256 live slots. A slot in bucket d names camera slot d * 1024 + camera_local. `camera_map`: each camera id appears once.
All inputs are finite; a program needn't handle non-finite values.
Results may differ from the reference program's by a relative error of at most 0.0003.
Values sent between devices are 32-bit elements; how exact they have to be, the bound alone decides.
A program may use at most 192 MiB of HBM per device.

```python
import math
import jax
import jax.numpy as jnp
import numpy as np
from jax import lax

CAM_DEV = 1024
CAP = 512
CAM = 8192
SLOTS = 131072
N_OBS = 8
N_REP = 4


def draw_bucket_counts(key, part):
    key_hot = jax.random.fold_in(key, 11)
    key_full = jax.random.fold_in(key, 12)
    key_base = jax.random.fold_in(key, 13)
    hotness = jax.random.randint(key_hot, (N_OBS,), 1, 4)
    full_column = jax.random.randint(key_full, (), 0, N_OBS)
    baseline = jax.random.randint(key_base, (N_OBS * N_REP, N_OBS), CAP // 4, CAP // 2 + 1)
    counts = jnp.minimum(CAP // 2, baseline * hotness[None, :] // 2)
    counts = jnp.maximum(counts, 1)
    column_ids = jnp.arange(N_OBS, dtype=jnp.int32)
    counts = jnp.where(column_ids[None, :] == full_column, CAP, counts)
    return counts.astype(jnp.int32)


def set_ends(drawn, rng, low, largest):
    index_at = [jax.random.randint(jax.random.fold_in(rng, axis), (), 0, length) for axis, length in enumerate(drawn.shape)]
    widest = drawn.shape.index(max(drawn.shape))
    neighbour = index_at[:widest] + [(index_at[widest] + 1) % drawn.shape[widest]] + index_at[widest + 1:]
    return drawn.at[tuple(index_at)].set(low).at[tuple(neighbour)].set(largest)


def block_scale(rng, dims, pieces, smallest, high):
    level, own = 1.0, jax.random.fold_in(rng, 6)
    for dim, shards_of in pieces:
        heights = jnp.exp(jax.random.uniform(jax.random.fold_in(own, dim), (shards_of,), jnp.float32, smallest / len(pieces), high / len(pieces)))
        level = level * jnp.repeat(heights, dims[dim] // shards_of).reshape([-1 if axis == dim else 1 for axis in range(len(dims))])
    return level


def rank_bounds(amount, skew):
    loads = [(1 << 20) // math.isqrt(grade ** skew) + 1 for grade in range(1, amount + 1)]
    scale = 1 + sum(loads) // (1 << 30)
    return np.cumsum(np.array([max(1, weight // scale) for weight in loads]))


def ranked_ids(key, dims, count, lean):
    grid = rank_bounds(count, lean)
    ticket = jax.random.randint(jax.random.fold_in(key, 1), dims, 0, int(grid[count - 1]))
    grade = jnp.searchsorted(jnp.asarray(grid, jnp.int32), ticket, side="right")
    return jax.random.permutation(jax.random.fold_in(key, 2), count)[grade].astype(jnp.int32)


def normal_values(rng, shape, width, most, shards=(), kind=jnp.bfloat16):
    level = block_scale(rng, shape, shards, -0.22, 0.18) if shards else 1.0
    values = jax.random.normal(rng, shape, jnp.float32) * width * level
    return jnp.minimum(jnp.maximum(values, -most), most).astype(kind)


def setup_inputs(seed: int = 0) -> dict:
    key_of = jax.random.split(jax.random.key(seed), 6)
    return {
        "jacobians": normal_values(key_of[0], (18, SLOTS), 0.5, 3.0, ((1, 32),), jnp.float32),
        "residuals": normal_values(key_of[1], (2, SLOTS), 1.0, 6.0, ((1, 32),), jnp.float32),
        "camera_local": set_ends(ranked_ids(key_of[2], (SLOTS,), CAM_DEV, 1), jax.random.fold_in(key_of[2], 3), 0, CAM_DEV - 1).astype(jnp.int32),
        "bucket_counts": draw_bucket_counts(jax.random.fold_in(key_of[5], 71), 0),
        "camera_map": jax.random.permutation(key_of[4], CAM).astype(jnp.int32),
    }


def observation_terms(jacobs, resids):
    leading_row = jacobs[0:9]
    trailing_row = jacobs[9:18]
    gradient_terms = leading_row * resids[0:1] + trailing_row * resids[1:2]
    block_terms = leading_row[:, None] * leading_row[None, :] + trailing_row[:, None] * trailing_row[None, :]
    block_terms = block_terms.reshape((81,) + leading_row.shape[1:])
    return jnp.concatenate([gradient_terms, block_terms], axis=0)


def reference(jacobians, residuals, camera_local, bucket_counts, camera_map):
    sources = N_OBS * N_REP
    columns = N_OBS * CAP
    jac_blocks = jnp.moveaxis(jacobians.reshape(18, sources, columns), 1, 0)
    res_blocks = jnp.moveaxis(residuals.reshape(2, sources, columns), 1, 0)
    cam_blocks = camera_local.reshape(sources, columns)
    position = jnp.arange(columns, dtype=jnp.int32)
    target = position // CAP
    within = position % CAP

    def accumulate(summed, inputs):
        jac_here, res_here, cam_here, count_here = inputs
        live_mask = (within < count_here[target]).astype(jnp.float32)
        obs_terms = observation_terms(jac_here * live_mask, res_here * live_mask)
        segment = (target * CAM_DEV + cam_here).astype(jnp.int32)
        return summed + jax.ops.segment_sum(obs_terms.T, segment, num_segments=CAM), None

    summed, unused = lax.scan(accumulate, jnp.zeros((CAM, 90), jnp.float32), (jac_blocks, res_blocks, cam_blocks, bucket_counts))
    slot_gradient = summed[:, :9].T
    camera_blocks = summed[:, 9:].T
    gradient = jnp.zeros((9, CAM), jnp.float32).at[:, camera_map].set(slot_gradient)
    return gradient, camera_blocks
```

```python
import functools

import jax
import jax.numpy as jnp
from jax import lax
from jax.experimental import pallas as pl
from jax.experimental.pallas import tpu as pltpu
from jax.sharding import PartitionSpec as P

CAM_DEV = 1024
MESH = pl.DeviceIdType.MESH
F32 = jnp.float32
BF16 = jnp.bfloat16
VMEM = pltpu.VMEM
KEPT = 48
LOW = 256
PAIR = 2
EARLY = 3
MIB = 1024 * 1024
DIMS = (((1,), (1,)), ((), ()))


def vspec():
    return pl.BlockSpec(memory_space=VMEM)


def xor(a, b, size):
    out, bit = 0, 1
    while bit < size:
        p, q = lax.rem(a // bit, 2), lax.rem(b // bit, 2)
        out = out + bit * (p + q - 2 * p * q)
        bit *= 2
    return out


def split(value):
    high = value.astype(BF16).astype(F32)
    return high, value - high


def pack(counts, jac, res, ids, own8, own2, tail):
    buckets = counts.shape[1]
    cap = jac.shape[1] // buckets
    tail[...] = jac[16:18, :]
    own8[...] = jac[0:8, :] * res[0:1, :] + jac[9:17, :] * res[1:2, :]
    own2[0:1, :] = jac[8:9, :] * res[0:1, :] + jac[17:18, :] * res[1:2, :]
    place = lax.broadcasted_iota(jnp.int32, (1, cap), 1)
    for d in range(buckets):
        lanes = slice(d * cap, (d + 1) * cap)
        own2[1:2, lanes] = jnp.where(place < counts[0, d], ids[:, lanes], -1).astype(F32)


def one_hot_of(low, wide):
    shape = (wide, low.shape[1])
    rows = lax.broadcasted_iota(jnp.int32, shape, 0).astype(F32).astype(BF16)
    there = jnp.broadcast_to(low.astype(F32), shape).astype(BF16)
    return jnp.where(there == rows, jnp.ones(shape, BF16), jnp.zeros(shape, BF16))


def place_of(pair, width):
    ids = pair[1:2].astype(jnp.int32)
    up = jnp.where(ids < 0, -1, ids // width)
    return up, ids - up * width


def masked_tiles(value, up, pieces):
    up = jnp.broadcast_to(up.astype(F32), value.shape).astype(BF16)
    zero = jnp.zeros_like(value)
    return [jnp.where(up == jnp.asarray(h, BF16), value, zero) for h in range(pieces)]


def add_gradient(eight, pair, hot, acc, pieces):
    up, down = place_of(pair, acc.shape[1])
    one_hot = one_hot_of(down, acc.shape[1])
    if hot is not None:
        hot[...] = one_hot
    high, low = split(eight)
    tiles = masked_tiles(jnp.concatenate([high, low], axis=0).astype(BF16), up, pieces)
    high, low = split(pair[0:1])
    mask = up == lax.broadcasted_iota(jnp.int32, (pieces, up.shape[1]), 0)
    last = jnp.concatenate([jnp.where(mask, high, 0.0), jnp.where(mask, low, 0.0)], axis=0).astype(BF16)
    lhs = jnp.concatenate(tiles + [last], axis=0)
    acc[...] += lax.dot_general(lhs, one_hot, DIMS, preferred_element_type=F32)


def add_block(most, tail, pair, hot, terms, acc):
    pieces, _, width = acc.shape
    lead, trail = most[0:9], jnp.concatenate([most[9:16], tail], axis=0)
    at = 0
    for k in range(9):
        terms[at : at + 9 - k, :] = lead[k : k + 1] * lead[k:9] + trail[k : k + 1] * trail[k:9]
        at += 9 - k
    high, low = split(terms[...])
    both = jnp.concatenate([high, low], axis=0).astype(BF16)
    up, down = place_of(pair, width)
    one_hot = one_hot_of(down, width) if hot is None else hot[...]
    lhs = jnp.concatenate(masked_tiles(both, up, pieces), axis=0)
    added = lax.dot_general(lhs, one_hot, DIMS, preferred_element_type=F32)
    for h in range(pieces):
        at = h * 2 * KEPT
        acc[h] += added[at : at + KEPT] + added[at + KEPT : at + 2 * KEPT]


def expand(blocks, out):
    m, _, width = blocks.shape
    at = 0
    for k in range(9):
        for l in range(k, 9):
            for r in range(m):
                row = blocks[r, at : at + 1, :]
                lanes = slice(r * width, (r + 1) * width)
                out[k * 9 + l : k * 9 + l + 1, lanes] = row
                if l != k:
                    out[l * 9 + k : l * 9 + k + 1, lanes] = row
            at += 1


def place_chunk(o, grads8, grads9, cmap, ready, acc):
    m, n, _, width = grads8.shape
    span = m * width
    highs = n * span // LOW
    eight = jnp.concatenate([grads8[r, o] for r in range(m)], axis=1)
    ninth = jnp.concatenate([grads9[r, o] for r in range(m)], axis=1)
    ids = cmap[:, pl.ds(pl.multiple_of(o * span, span), span)]
    up = ids // LOW
    one_hot = one_hot_of(lax.rem(ids, LOW), LOW) if ready is None else ready[o]
    high, low = split(eight)
    top = jnp.concatenate([high, low], axis=0).astype(BF16)
    up16 = jnp.broadcast_to(up.astype(F32), (16, span)).astype(BF16)
    none = jnp.zeros_like(top)
    mask = up == lax.broadcasted_iota(jnp.int32, (highs, span), 0)
    high, low = split(ninth)
    last = jnp.concatenate([jnp.where(mask, high, 0.0), jnp.where(mask, low, 0.0)], axis=0).astype(BF16)
    group = min(highs, 32)

    def tiles(start):
        return [jnp.where(up16 == jnp.asarray(start + h, F32).astype(BF16), top, none) for h in range(group)]

    if group == highs:
        lhs = jnp.concatenate(tiles(0) + [last], axis=0)
        acc[...] += lax.dot_general(lhs, one_hot, DIMS, preferred_element_type=F32)
        return

    def some(g, carry):
        lhs = jnp.concatenate(tiles(g * group), axis=0)
        where = pl.ds(pl.multiple_of(g * group * 16, group * 16), group * 16)
        acc[where, :] += lax.dot_general(lhs, one_hot, DIMS, preferred_element_type=F32)
        return carry

    lax.fori_loop(0, highs // group, some, 0)
    acc[highs * 16 :, :] += lax.dot_general(last, one_hot, DIMS, preferred_element_type=F32)


def lay_out(acc, gradient):
    highs = gradient.shape[1] // LOW
    for h in range(highs):
        lanes = slice(h * LOW, (h + 1) * LOW)
        gradient[0:8, lanes] = acc[h * 16 : h * 16 + 8, :] + acc[h * 16 + 8 : h * 16 + 16, :]
        ninth = highs * 16 + h
        gradient[8:9, lanes] = acc[ninth : ninth + 1, :] + acc[ninth + highs : ninth + highs + 1, :]


def main_kernel(
    n, m, counts, jac_in, res_in, ids_in, cmap_in, gradient, out, jac, res, ids, cmap, load_sem,
    own8, own2, tail, got8, got2, got16, got_tail, hots, terms, part, landed, total, blocks,
    gsum, part8, part9, land8, land9, mine8, mine9, grads8, grads9, ready, spread,
    x_send, x_recv, a_send, a_recv, g_send, g_recv, c_send, c_recv, b_send, b_recv, w_send, w_recv,
):
    me, rep = lax.axis_index("obs"), lax.axis_index("rep")
    width = total.shape[1]
    cap = got8.shape[2]
    half = m // PAIR
    sibling = rep + 1 - 2 * lax.rem(rep, PAIR)
    barrier = pltpu.get_barrier_semaphore()

    def greet(i, carry):
        for j in range(half):
            where = {"obs": xor(me, i, n), "rep": lax.rem(rep + PAIR * j, m)}
            pl.semaphore_signal(barrier, inc=1, device_id=where, device_id_type=MESH)
        return carry

    lax.fori_loop(1, n, greet, 0)
    for i in range(1, m):
        pl.semaphore_signal(barrier, inc=1, device_id={"rep": lax.rem(rep + i, m)}, device_id_type=MESH)
    pairs = ((jac_in, jac), (res_in, res), (ids_in, ids), (cmap_in, cmap))
    loads = [pltpu.make_async_copy(src, dst, load_sem.at[k]) for k, (src, dst) in enumerate(pairs)]
    for load in loads:
        load.start()
    part[...] = jnp.zeros_like(part)
    terms[...] = jnp.zeros_like(terms)
    gsum[...] = jnp.zeros_like(gsum)
    spread[...] = jnp.zeros_like(spread)
    for load in loads:
        load.wait()
    pack(counts, jac, res, ids, own8, own2, tail)
    pl.semaphore_wait(barrier, (n - 1) * half + m - 1)

    def lanes_of(peer):
        return pl.ds(pl.multiple_of(peer * cap, cap), cap)

    def handing(i, kinds):
        peer = xor(me, i, n)
        lanes = lanes_of(peer)
        sent = (own8.at[:, lanes], own2.at[:, lanes], jac.at[0:16, lanes], tail.at[:, lanes])
        taken = (got8.at[i], got2.at[i], got16.at[i], got_tail.at[i])
        return [
            pltpu.make_async_remote_copy(
                src_ref=sent[k], dst_ref=taken[k], send_sem=x_send.at[k, i], recv_sem=x_recv.at[k, i],
                device_id={"obs": peer}, device_id_type=MESH,
            )
            for k in kinds
        ]

    def start(kinds):
        def one(i, carry):
            for copy in handing(n - i, kinds):
                copy.start()
            return carry

        lax.fori_loop(1, n, one, 0)

    start((0, 1))
    start((2, 3))
    early = ready.shape[0] == n

    def hot_at(i):
        return hots.at[i] if early else None

    def prepare(o, carry):
        ids_here = cmap[:, pl.ds(pl.multiple_of(o * m * width, m * width), m * width)]
        ready[o] = one_hot_of(lax.rem(ids_here, LOW), LOW)
        return carry

    def take_gradient(i, carry):
        for copy in handing(i, (0, 1)):
            copy.wait_recv()
        add_gradient(got8[i], got2[i], hot_at(i), gsum, m)
        return carry

    def take_block(i, carry):
        for copy in handing(i, (2, 3)):
            copy.wait_recv()
        add_block(got16[i], got_tail[i], got2[i], hot_at(i), terms, part)
        return carry

    mylanes = lanes_of(me)
    add_gradient(own8[:, mylanes], own2[:, mylanes], hot_at(0), gsum, m)
    if early:
        lax.fori_loop(0, n, prepare, 0)
    lax.fori_loop(1, n, take_gradient, 0)
    for h in range(m):
        part8[h] = gsum[h * 16 : h * 16 + 8, :] + gsum[h * 16 + 8 : h * 16 + 16, :]
        ninth = m * 16 + h
        part9[h] = gsum[ninth : ninth + 1, :] + gsum[ninth + m : ninth + m + 1, :]

    def to_rep(src, dst, s, r, peer):
        return pltpu.make_async_remote_copy(
            src_ref=src, dst_ref=dst, send_sem=s, recv_sem=r, device_id={"rep": peer}, device_id_type=MESH
        )

    heads = []
    for i in range(1, m):
        peer = lax.rem(rep + i, m)
        heads.append(to_rep(part8.at[peer], land8.at[i], a_send.at[0, i], a_recv.at[0, i], peer))
        heads.append(to_rep(part9.at[peer], land9.at[i], a_send.at[1, i], a_recv.at[1, i], peer))
    for copy in heads:
        copy.start()
    add_block(jac[0:16, mylanes], tail[:, mylanes], own2[:, mylanes], hot_at(0), terms, part)
    lax.fori_loop(1, min(EARLY, n), take_block, 0)
    for copy in heads:
        copy.wait_recv()
    eight, ninth = part8[rep], part9[rep]
    for i in range(1, m):
        eight = eight + land8[i]
        ninth = ninth + land9[i]
    mine8[...] = eight
    mine9[...] = ninth
    grads8[rep, me] = eight
    grads9[rep, me] = ninth

    def at_origin(origin, source):
        return grads8.at[origin, source], grads9.at[origin, source]

    def reach(i, j):
        where = {"obs": xor(me, i, n), "rep": lax.rem(rep + PAIR * j, m)}
        return [
            pltpu.make_async_remote_copy(
                src_ref=src, dst_ref=dst, send_sem=g_send.at[k, i, j], recv_sem=g_recv.at[k, i, j],
                device_id=where, device_id_type=MESH,
            )
            for k, (src, dst) in enumerate(zip((mine8, mine9), at_origin(rep, me)))
        ]

    def hand_over(i, j, src, dst):
        return [to_rep(src[k], dst[k], c_send.at[k, i, j], c_recv.at[k, i, j], sibling) for k in range(2)]

    def spread_out(i, carry):
        for j in reversed(range(half)):
            for copy in reach(n - i, j):
                copy.start()
        return carry

    lax.fori_loop(1, n, spread_out, 0)
    for j in range(1, half):
        for copy in reach(0, j):
            copy.start()
    for copy in hand_over(0, 0, (mine8, mine9), at_origin(rep, me)):
        copy.start()
    lax.fori_loop(min(EARLY, n), n, take_block, 0)
    folds = []
    for i in range(1, m):
        peer = lax.rem(rep + i, m)
        folds.append(to_rep(part.at[peer], landed.at[i], b_send.at[i], b_recv.at[i], peer))
    for copy in folds:
        copy.start()

    def relay(i, first):
        source = xor(me, i, n)
        for j in range(first, half):
            for copy in reach(i, j):
                copy.wait_recv()
            piece = at_origin(lax.rem(rep - PAIR * j + m, m), source)
            for copy in hand_over(i, j, piece, piece):
                copy.start()

    def relay_all(i, carry):
        relay(i, 0)
        return carry

    def place(i, carry):
        source = xor(me, i, n)
        for j in range(half):
            piece = at_origin(lax.rem(sibling - PAIR * j + m, m), source)
            for copy in hand_over(i, j, piece, piece):
                copy.wait_recv()
        place_chunk(source, grads8, grads9, cmap, ready if early else None, spread)
        return carry

    relay(0, 1)
    for copy in folds:
        copy.wait_recv()
    rest = part[rep]
    for i in range(1, m):
        rest = rest + landed[i]
    total[...] = rest
    blocks[rep] = rest
    wide = []
    for j in range(1, m):
        peer = lax.rem(rep + j, m)
        wide.append(to_rep(total, blocks.at[rep], w_send.at[j], w_recv.at[j], peer))
    for copy in wide:
        copy.start()
    lax.fori_loop(1, n, relay_all, 0)
    lax.fori_loop(0, n, place, 0)
    lay_out(spread, gradient)
    for copy in wide:
        copy.wait_recv()
    expand(blocks, out)

    def finish(i, carry):
        for j in range(half):
            piece = at_origin(rep, me)
            for copy in hand_over(i, j, piece, piece):
                copy.wait_send()
        return carry

    def finish_far(i, carry):
        for copy in handing(i, (0, 1, 2, 3)):
            copy.wait_send()
        for j in range(half):
            for copy in reach(i, j):
                copy.wait_send()
        return carry

    lax.fori_loop(0, n, finish, 0)
    lax.fori_loop(1, n, finish_far, 0)
    for j in range(1, half):
        for copy in reach(0, j):
            copy.wait_send()
    for copy in heads + folds + wide:
        copy.wait_send()


def write_kernel(gradient, blocks, gradient_out, blocks_out, out_sem):
    def cut(ref, count):
        step = ref.shape[1] // count
        return [ref.at[:, pl.ds(c * step, step)] for c in range(count)]

    jobs = list(zip(cut(blocks, 2), cut(blocks_out, 2)))
    jobs += list(zip(cut(gradient, 4), cut(gradient_out, 4)))
    writes = [pltpu.make_async_copy(job[0], job[1], out_sem.at[j]) for j, job in enumerate(jobs)]
    for write in writes:
        write.start()
    for write in writes:
        write.wait()


def local(jacobians, residuals, camera_local, bucket_counts, camera_map):
    n, m = lax.axis_size("obs"), lax.axis_size("rep")
    slots = jacobians.shape[1]
    cap = slots // n
    cams = camera_map.shape[0]
    width = CAM_DEV // m
    highs = cams // LOW
    half = m // PAIR
    dma = pltpu.SemaphoreType.DMA
    early = n * LOW * CAM_DEV * 2 <= 8 * MIB
    kept = n if early else 1
    held = 16 * cams * 4 + 88 * CAM_DEV * 4
    limit = 60 * MIB - max(0, held - 2 * MIB)
    gradient, out = pl.pallas_call(
        functools.partial(main_kernel, n, m),
        out_shape=(VMEM((9, cams), F32), VMEM((81, CAM_DEV), F32)),
        in_specs=[pl.BlockSpec(memory_space=pltpu.SMEM)] + [pl.BlockSpec(memory_space=pltpu.HBM)] * 4,
        out_specs=(vspec(), vspec()),
        scratch_shapes=[
            VMEM((18, slots), F32),
            VMEM((2, slots), F32),
            VMEM((1, slots), jnp.int32),
            VMEM((1, cams), jnp.int32),
            dma((4,)),
            VMEM((8, slots), F32),
            VMEM((2, slots), F32),
            VMEM((2, slots), F32),
            VMEM((n, 8, cap), F32),
            VMEM((n, 2, cap), F32),
            VMEM((n, 16, cap), F32),
            VMEM((n, 2, cap), F32),
            VMEM((kept, width, cap), BF16),
            VMEM((KEPT, cap), F32),
            VMEM((m, KEPT, width), F32),
            VMEM((m, KEPT, width), F32),
            VMEM((KEPT, width), F32),
            VMEM((m, KEPT, width), F32),
            VMEM((m * 18, width), F32),
            VMEM((m, 8, width), F32),
            VMEM((m, 1, width), F32),
            VMEM((m, 8, width), F32),
            VMEM((m, 1, width), F32),
            VMEM((8, width), F32),
            VMEM((1, width), F32),
            VMEM((m, n, 8, width), F32),
            VMEM((m, n, 1, width), F32),
            VMEM((kept, LOW, CAM_DEV), BF16),
            VMEM((highs * 18, LOW), F32),
            dma((4, n)),
            dma((4, n)),
            dma((2, m)),
            dma((2, m)),
            dma((2, n, half)),
            dma((2, n, half)),
            dma((2, n, half)),
            dma((2, n, half)),
            dma((m,)),
            dma((m,)),
            dma((m,)),
            dma((m,)),
        ],
        compiler_params=pltpu.CompilerParams(collective_id=0, has_side_effects=True, vmem_limit_bytes=limit),
    )(bucket_counts, jacobians, residuals, camera_local.reshape(1, slots), camera_map.reshape(1, cams))
    anywhere = pl.BlockSpec(memory_space=pl.ANY)
    shapes = (jax.ShapeDtypeStruct(gradient.shape, F32), jax.ShapeDtypeStruct(out.shape, F32))
    return pl.pallas_call(
        write_kernel,
        out_shape=shapes,
        in_specs=[vspec()] * 2,
        out_specs=(anywhere, anywhere),
        scratch_shapes=[dma((6,))],
        compiler_params=pltpu.CompilerParams(vmem_limit_bytes=2 * MIB),
    )(gradient, out)


def solution(mesh):
    in_specs = (
        P(None, ("obs", "rep")),
        P(None, ("obs", "rep")),
        P(("obs", "rep")),
        P(("obs", "rep"), None),
        P(),
    )
    out_specs = (P(), P(None, "obs"))
    return jax.shard_map(local, mesh=mesh, in_specs=in_specs, out_specs=out_specs, check_vma=False)
```

```python
import functools

import jax
import jax.numpy as jnp
from jax import lax
from jax.experimental import pallas as pl
from jax.experimental.pallas import tpu as pltpu
from jax.sharding import PartitionSpec as P

CAM_DEV = 1024
MESH = pl.DeviceIdType.MESH
F32 = jnp.float32
BF16 = jnp.bfloat16
VMEM = pltpu.VMEM
ROWS = 56
KEPT = 48
CUTS = 4
LOW = 256
PAIR = 2
MIB = 1024 * 1024
DIMS = (((1,), (1,)), ((), ()))


def vspec():
    return pl.BlockSpec(memory_space=VMEM)


def flipper(me, size):
    weights = [1 << k for k in range(size.bit_length() - 1)]
    signed = [w * (1 - 2 * lax.rem(me // w, 2)) for w in weights]

    def flip(i):
        out = me
        for w, s in zip(weights, signed):
            if isinstance(i, int):
                out = out + s if i // w % 2 else out
            else:
                out = out + s * lax.rem(lax.div(i, w), 2)
        return out

    return flip


def each(first, last, body):
    if last - first <= 8:
        for i in range(first, last):
            body(i)
    else:
        lax.fori_loop(first, last, lambda i, carry: (body(i), carry)[1], 0)


def split(value):
    high = value.astype(BF16).astype(F32)
    return high, value - high


def pack(counts, jac, res, ids, own4, own1):
    buckets = counts.shape[1]
    cap = jac.shape[1] // buckets
    own4[0:2, :] = jac[16:18, :]
    own4[2:4, :] = res[...]
    place = lax.broadcasted_iota(jnp.int32, (1, cap), 1)
    for d in range(buckets):
        lanes = slice(d * cap, (d + 1) * cap)
        own1[:, lanes] = jnp.where(place < counts[0, d], ids[:, lanes], -1).astype(F32)


def one_hot_of(low, wide):
    shape = (wide, low.shape[1])
    rows = lax.broadcasted_iota(jnp.int32, shape, 0).astype(F32).astype(BF16)
    there = jnp.broadcast_to(low.astype(F32), shape).astype(BF16)
    return jnp.where(there == rows, jnp.ones(shape, BF16), jnp.zeros(shape, BF16))


def place_of(ids, width):
    ids = ids.astype(jnp.int32)
    up = jnp.where(ids < 0, -1, ids // width)
    return up, ids - up * width


def masked_tiles(value, up, pieces):
    up = jnp.broadcast_to(up.astype(F32), value.shape).astype(BF16)
    zero = jnp.zeros_like(value)
    return [jnp.where(up == jnp.asarray(h, BF16), value, zero) for h in range(pieces)]


def add_block(most, four, ids, hot, terms, acc):
    pieces, _, width = acc.shape
    lead, trail, res = most[0:9], jnp.concatenate([most[9:16], four[0:2]], axis=0), four[2:4]
    at = 9
    for k in range(9):
        terms[at : at + 9 - k, :] = lead[k : k + 1] * lead[k:9] + trail[k : k + 1] * trail[k:9]
        at += 9 - k
    terms[0:9, :] = lead * res[0:1] + trail * res[1:2]
    high, low = split(terms[...])
    both = jnp.concatenate([high, low], axis=0).astype(BF16)
    up, down = place_of(ids, width)
    one_hot = one_hot_of(down, width) if hot is None else hot[...]
    lhs = jnp.concatenate(masked_tiles(both, up, pieces), axis=0)
    added = lax.dot_general(lhs, one_hot, DIMS, preferred_element_type=F32)
    for h in range(pieces):
        at = h * 2 * ROWS
        acc[h] += added[at : at + ROWS] + added[at + ROWS : at + 2 * ROWS]


def expand(blocks, out):
    m, _, width = blocks.shape
    at = 1
    for k in range(9):
        for l in range(k, 9):
            for r in range(m):
                row = blocks[r, at : at + 1, :]
                lanes = slice(r * width, (r + 1) * width)
                out[k * 9 + l : k * 9 + l + 1, lanes] = row
                if l != k:
                    out[l * 9 + k : l * 9 + k + 1, lanes] = row
            at += 1


def side_ids(o, side, pieces, cmap, width):
    m = PAIR * pieces

    def at(j):
        return pl.ds(pl.multiple_of((o * m + side + PAIR * j) * width, width), width)

    return jnp.concatenate([cmap[:, at(j)] for j in range(pieces)], axis=1)


def place_chunk(eight, ninth, ids, one_hot, acc):
    span = ids.shape[1]
    highs = acc.shape[0] // 18
    up = ids // LOW
    if one_hot is None:
        one_hot = one_hot_of(lax.rem(ids, LOW), LOW)
    high, low = split(eight)
    top = jnp.concatenate([high, low], axis=0).astype(BF16)
    up16 = jnp.broadcast_to(up.astype(F32), (16, span)).astype(BF16)
    none = jnp.zeros_like(top)
    mask = up == lax.broadcasted_iota(jnp.int32, (highs, span), 0)
    high, low = split(ninth)
    last = jnp.concatenate([jnp.where(mask, high, 0.0), jnp.where(mask, low, 0.0)], axis=0).astype(BF16)
    group = min(highs, 32)

    def tiles(start):
        return [jnp.where(up16 == jnp.asarray(start + h, F32).astype(BF16), top, none) for h in range(group)]

    if group == highs:
        lhs = jnp.concatenate(tiles(0) + [last], axis=0)
        acc[...] += lax.dot_general(lhs, one_hot, DIMS, preferred_element_type=F32)
        return

    def some(g, carry):
        lhs = jnp.concatenate(tiles(g * group), axis=0)
        where = pl.ds(pl.multiple_of(g * group * 16, group * 16), group * 16)
        acc[where, :] += lax.dot_general(lhs, one_hot, DIMS, preferred_element_type=F32)
        return carry

    lax.fori_loop(0, highs // group, some, 0)
    acc[highs * 16 :, :] += lax.dot_general(last, one_hot, DIMS, preferred_element_type=F32)


def lay_out(acc, out8, out9, first, last):
    highs = out8.shape[1] // LOW
    for h in range(first, last):
        lanes = slice(h * LOW, (h + 1) * LOW)
        out8[:, lanes] = acc[h * 16 : h * 16 + 8, :] + acc[h * 16 + 8 : h * 16 + 16, :]
        ninth = highs * 16 + h
        out9[:, lanes] = acc[ninth : ninth + 1, :] + acc[ninth + highs : ninth + highs + 1, :]


def main_kernel(
    n, m, counts, jac_in, res_in, ids_in, cmap_in, gradient, out, jac, res, ids, cmap, load_sem,
    own4, own1, got16, got4, got1, hots, terms, part, fold, landed, total, blocks,
    part8, part9, land8, land9, mine8, mine9, grads8, grads9, ready, spread, out8, out9, sib8, sib9,
    x_send, x_recv, a_send, a_recv, g_send, g_recv, c_send, c_recv, b_send, b_recv, w_send, w_recv, d_send, d_recv,
):
    me, rep = lax.axis_index("obs"), lax.axis_index("rep")
    width = total.shape[2]
    cap = got16.shape[2]
    half = m // PAIR
    sibling = rep + 1 - 2 * lax.rem(rep, PAIR)
    barrier = pltpu.get_barrier_semaphore()

    flip = flipper(me, n)

    def greet(i):
        pl.semaphore_signal(barrier, inc=1, device_id={"obs": flip(i)}, device_id_type=MESH)

    each(1, n, greet)
    for i in range(1, m):
        pl.semaphore_signal(barrier, inc=1, device_id={"rep": lax.rem(rep + i, m)}, device_id_type=MESH)
    pairs = ((jac_in, jac), (res_in, res), (ids_in, ids), (cmap_in, cmap))
    loads = [pltpu.make_async_copy(src, dst, load_sem.at[k]) for k, (src, dst) in enumerate(pairs)]
    for load in loads:
        load.start()
    part[...] = jnp.zeros_like(part)
    terms[...] = jnp.zeros_like(terms)
    spread[...] = jnp.zeros_like(spread)
    for load in loads:
        load.wait()
    pack(counts, jac, res, ids, own4, own1)
    pl.semaphore_wait(barrier, n + m - 2)

    def lanes_of(peer):
        return pl.ds(pl.multiple_of(peer * cap, cap), cap)

    def handing(i, kinds):
        peer = flip(i)
        lanes = lanes_of(peer)
        sent = (own1.at[:, lanes], jac.at[0:16, lanes], own4.at[:, lanes])
        taken = (got1.at[i], got16.at[i], got4.at[i])
        return [
            pltpu.make_async_remote_copy(
                src_ref=sent[k], dst_ref=taken[k], send_sem=x_send.at[k, i], recv_sem=x_recv.at[k, i],
                device_id={"obs": peer}, device_id_type=MESH,
            )
            for k in kinds
        ]

    def start(kinds):
        def one(i):
            for copy in handing(n - i, kinds):
                copy.start()

        each(1, n, one)

    start((0,))
    start((1, 2))
    early = ready.shape[0] == n

    def hot_at(i):
        return hots.at[i] if early else None

    side = lax.rem(rep, PAIR)

    def prepare(o, carry):
        ready[o] = one_hot_of(lax.rem(side_ids(o, side, half, cmap, width), LOW), LOW)
        return carry

    def foresee(i, carry):
        for copy in handing(i, (0,)):
            copy.wait_recv()
        if early:
            hots[i] = one_hot_of(place_of(got1[i], width)[1], width)
        return carry

    def take(i, carry):
        for copy in handing(i, (1, 2)):
            copy.wait_recv()
        add_block(got16[i], got4[i], got1[i], hot_at(i), terms, part)
        return carry

    mylanes = lanes_of(me)
    add_block(jac[0:16, mylanes], own4[:, mylanes], own1[:, mylanes], None, terms, part)
    lax.fori_loop(1, n, foresee, 0)
    if early:
        lax.fori_loop(0, n, prepare, 0)
    lax.fori_loop(1, n, take, 0)
    for h in range(m):
        part8[h] = part[h, 0:8]
        part9[h] = part[h, 8:9]

    def to_rep(src, dst, s, r, peer):
        return pltpu.make_async_remote_copy(
            src_ref=src, dst_ref=dst, send_sem=s, recv_sem=r, device_id={"rep": peer}, device_id_type=MESH
        )

    heads = []
    for i in range(1, m):
        peer = lax.rem(rep + i, m)
        heads.append(to_rep(part8.at[peer], land8.at[i], a_send.at[0, i], a_recv.at[0, i], peer))
        heads.append(to_rep(part9.at[peer], land9.at[i], a_send.at[1, i], a_recv.at[1, i], peer))
    for copy in heads:
        copy.start()
    mine_at, other_at = side * half, (1 - side) * half
    folds, wide, back = [], [], []
    for h in range(half):
        folds.append(to_rep(part.at[other_at + h, pl.ds(ROWS - KEPT, KEPT)], fold.at[h], b_send.at[h], b_recv.at[h], sibling))
        for j in range(1, half):
            peer = lax.rem(rep + PAIR * j, m)
            wide.append(to_rep(total.at[h], landed.at[j, h], w_send.at[j, h], w_recv.at[j, h], peer))
        back.append(to_rep(blocks.at[mine_at + h], blocks.at[mine_at + h], d_send.at[h], d_recv.at[h], sibling))
    for copy in folds:
        copy.start()
    for copy in heads:
        copy.wait_recv()
    eight, ninth = part8[rep], part9[rep]
    for i in range(1, m):
        eight = eight + land8[i]
        ninth = ninth + land9[i]
    mine8[...] = eight
    mine9[...] = ninth
    grads8[lax.div(rep, PAIR), me] = eight
    grads9[lax.div(rep, PAIR), me] = ninth

    def at_origin(origin, source):
        return grads8.at[origin, source], grads9.at[origin, source]

    def reach(i, j):
        where = {"obs": flip(i), "rep": lax.rem(rep + PAIR * j, m)}
        return [
            pltpu.make_async_remote_copy(
                src_ref=src, dst_ref=dst, send_sem=g_send.at[k, i, j], recv_sem=g_recv.at[k, i, j],
                device_id=where, device_id_type=MESH,
            )
            for k, (src, dst) in enumerate(zip((mine8, mine9), at_origin(lax.div(rep, PAIR), me)))
        ]

    def spread_out(i):
        for j in reversed(range(half)):
            for copy in reach(n - i, j):
                copy.start()

    each(1, n, spread_out)
    for j in range(1, half):
        for copy in reach(0, j):
            copy.start()

    def place(i, first):
        source = flip(i)
        for j in range(first, half):
            for copy in reach(i, j):
                copy.wait_recv()
        eight = jnp.concatenate([grads8[j, source] for j in range(half)], axis=1)
        ninth = jnp.concatenate([grads9[j, source] for j in range(half)], axis=1)
        here = side_ids(source, side, half, cmap, width)
        place_chunk(eight, ninth, here, ready[source] if early else None, spread)

    def settle(i, carry):
        place(i, 0)
        return carry

    for h in range(half):
        folds[h].wait_recv()
        total[h] = part[mine_at + h, ROWS - KEPT :] + fold[h]
        for copy in wide[h * (half - 1) : (h + 1) * (half - 1)]:
            copy.start()
    place(0, 1)
    lax.fori_loop(1, n, settle, 0)
    swaps = []
    highs, step = gradient.shape[1] // LOW, gradient.shape[1] // CUTS
    for c in range(CUTS):
        lanes = pl.ds(c * step, step)
        lay_out(spread, out8, out9, c * highs // CUTS, (c + 1) * highs // CUTS)
        swaps.append(to_rep(out8.at[:, lanes], sib8.at[:, lanes], c_send.at[0, c], c_recv.at[0, c], sibling))
        swaps.append(to_rep(out9.at[:, lanes], sib9.at[:, lanes], c_send.at[1, c], c_recv.at[1, c], sibling))
        for copy in swaps[-2:]:
            copy.start()
    for h in range(half):
        for copy in wide[h * (half - 1) : (h + 1) * (half - 1)]:
            copy.wait_recv()
        full = total[h]
        for j in range(1, half):
            full = full + landed[j, h]
        blocks[mine_at + h] = full
        back[h].start()
    for c in range(CUTS):
        lanes = slice(c * step, (c + 1) * step)
        for copy in swaps[2 * c : 2 * c + 2]:
            copy.wait_recv()
        gradient[0:8, lanes] = out8[:, lanes] + sib8[:, lanes]
        gradient[8:9, lanes] = out9[:, lanes] + sib9[:, lanes]
    for copy in back:
        copy.wait_recv()
    expand(blocks, out)

    def finish(i):
        for copy in handing(i, (0, 1, 2)):
            copy.wait_send()
        for j in range(half):
            for copy in reach(i, j):
                copy.wait_send()

    each(1, n, finish)
    for j in range(1, half):
        for copy in reach(0, j):
            copy.wait_send()
    for copy in heads + folds + wide + back + swaps:
        copy.wait_send()


def write_kernel(gradient, blocks, gradient_out, blocks_out, out_sem):
    def cut(ref, count):
        step = ref.shape[1] // count
        return [ref.at[:, pl.ds(c * step, step)] for c in range(count)]

    jobs = list(zip(cut(blocks, 2), cut(blocks_out, 2)))
    jobs += list(zip(cut(gradient, 4), cut(gradient_out, 4)))
    writes = [pltpu.make_async_copy(job[0], job[1], out_sem.at[j]) for j, job in enumerate(jobs)]
    for write in writes:
        write.start()
    for write in writes:
        write.wait()


def local(jacobians, residuals, camera_local, bucket_counts, camera_map):
    n, m = lax.axis_size("obs"), lax.axis_size("rep")
    slots = jacobians.shape[1]
    cap = slots // n
    cams = camera_map.shape[0]
    width = CAM_DEV // m
    highs = cams // LOW
    half = m // PAIR
    dma = pltpu.SemaphoreType.DMA
    early = n * LOW * CAM_DEV * 2 <= 8 * MIB
    kept = n if early else 1
    held = 16 * cams * 4 + 88 * CAM_DEV * 4
    limit = 60 * MIB - max(0, held - 2 * MIB)
    gradient, out = pl.pallas_call(
        functools.partial(main_kernel, n, m),
        out_shape=(VMEM((9, cams), F32), VMEM((81, CAM_DEV), F32)),
        in_specs=[pl.BlockSpec(memory_space=pltpu.SMEM)] + [pl.BlockSpec(memory_space=pltpu.HBM)] * 4,
        out_specs=(vspec(), vspec()),
        scratch_shapes=[
            VMEM((18, slots), F32),
            VMEM((2, slots), F32),
            VMEM((1, slots), jnp.int32),
            VMEM((1, cams), jnp.int32),
            dma((4,)),
            VMEM((4, slots), F32),
            VMEM((1, slots), F32),
            VMEM((n, 16, cap), F32),
            VMEM((n, 4, cap), F32),
            VMEM((n, 1, cap), F32),
            VMEM((kept, width, cap), BF16),
            VMEM((ROWS, cap), F32),
            VMEM((m, ROWS, width), F32),
            VMEM((half, KEPT, width), F32),
            VMEM((half, half, KEPT, width), F32),
            VMEM((half, KEPT, width), F32),
            VMEM((m, KEPT, width), F32),
            VMEM((m, 8, width), F32),
            VMEM((m, 1, width), F32),
            VMEM((m, 8, width), F32),
            VMEM((m, 1, width), F32),
            VMEM((8, width), F32),
            VMEM((1, width), F32),
            VMEM((half, n, 8, width), F32),
            VMEM((half, n, 1, width), F32),
            VMEM((kept, LOW, half * width), BF16),
            VMEM((highs * 18, LOW), F32),
            VMEM((8, cams), F32),
            VMEM((1, cams), F32),
            VMEM((8, cams), F32),
            VMEM((1, cams), F32),
            dma((3, n)),
            dma((3, n)),
            dma((2, m)),
            dma((2, m)),
            dma((2, n, half)),
            dma((2, n, half)),
            dma((2, CUTS)),
            dma((2, CUTS)),
            dma((half,)),
            dma((half,)),
            dma((half, half)),
            dma((half, half)),
            dma((half,)),
            dma((half,)),
        ],
        compiler_params=pltpu.CompilerParams(collective_id=0, has_side_effects=True, vmem_limit_bytes=limit),
    )(bucket_counts, jacobians, residuals, camera_local.reshape(1, slots), camera_map.reshape(1, cams))
    anywhere = pl.BlockSpec(memory_space=pl.ANY)
    shapes = (jax.ShapeDtypeStruct(gradient.shape, F32), jax.ShapeDtypeStruct(out.shape, F32))
    return pl.pallas_call(
        write_kernel,
        out_shape=shapes,
        in_specs=[vspec()] * 2,
        out_specs=(anywhere, anywhere),
        scratch_shapes=[dma((6,))],
        compiler_params=pltpu.CompilerParams(vmem_limit_bytes=2 * MIB),
    )(gradient, out)


def solution(mesh):
    in_specs = (
        P(None, ("obs", "rep")),
        P(None, ("obs", "rep")),
        P(("obs", "rep")),
        P(("obs", "rep"), None),
        P(),
    )
    out_specs = (P(), P(None, "obs"))
    return jax.shard_map(local, mesh=mesh, in_specs=in_specs, out_specs=out_specs, check_vma=False)
```

```python
import functools

import jax
import jax.numpy as jnp
from jax import lax
from jax.experimental import pallas as pl
from jax.experimental.pallas import tpu as pltpu
from jax.sharding import PartitionSpec as P

CAM_DEV = 1024
MESH = pl.DeviceIdType.MESH
F32 = jnp.float32
BF16 = jnp.bfloat16
VMEM = pltpu.VMEM
KEPT = 48
CUTS = 4
EARLY = 1
INLINE = 1
LOW = 256
PAIR = 2
MIB = 1024 * 1024
DIMS = (((1,), (1,)), ((), ()))


def vspec():
    return pl.BlockSpec(memory_space=VMEM)


def flipper(me, size):
    weights = [1 << k for k in range(size.bit_length() - 1)]
    signed = [w * (1 - 2 * lax.rem(me // w, 2)) for w in weights]

    def flip(i):
        out = me
        for w, s in zip(weights, signed):
            if isinstance(i, int):
                out = out + s if i // w % 2 else out
            else:
                out = out + s * lax.rem(lax.div(i, w), 2)
        return out

    return flip


def each(first, last, body):
    if last - first <= 8:
        for i in range(first, last):
            body(i)
    else:
        lax.fori_loop(first, last, lambda i, carry: (body(i), carry)[1], 0)


def split(value):
    high = value.astype(BF16).astype(F32)
    return high, value - high


def pack(counts, jac, res, ids, tail, own4, own2, own8):
    buckets = counts.shape[1]
    cap = jac.shape[1] // buckets
    tail[...] = jac[16:18, :]
    own4[0:2, :] = jac[16:18, :]
    own4[2:4, :] = res[...]
    own8[...] = jac[0:8, :] * res[0:1, :] + jac[9:17, :] * res[1:2, :]
    own2[1:2, :] = jac[8:9, :] * res[0:1, :] + jac[17:18, :] * res[1:2, :]
    place = lax.broadcasted_iota(jnp.int32, (1, cap), 1)
    for d in range(buckets):
        lanes = slice(d * cap, (d + 1) * cap)
        own2[0:1, lanes] = jnp.where(place < counts[0, d], ids[:, lanes], -1).astype(F32)


def one_hot_of(low, wide):
    shape = (wide, low.shape[1])
    rows = lax.broadcasted_iota(jnp.int32, shape, 0).astype(F32).astype(BF16)
    there = jnp.broadcast_to(low.astype(F32), shape).astype(BF16)
    return jnp.where(there == rows, jnp.ones(shape, BF16), jnp.zeros(shape, BF16))


def place_of(ids, width):
    ids = ids.astype(jnp.int32)
    up = jnp.where(ids < 0, -1, ids // width)
    return up, ids - up * width


def masked_tiles(value, up, pieces):
    up = jnp.broadcast_to(up.astype(F32), value.shape).astype(BF16)
    zero = jnp.zeros_like(value)
    return [jnp.where(up == jnp.asarray(h, BF16), value, zero) for h in range(pieces)]


def add_gradient(eight, pair, one_hot, acc, pieces):
    up, _ = place_of(pair[0:1], acc.shape[1])
    high, low = split(eight)
    tiles = masked_tiles(jnp.concatenate([high, low], axis=0).astype(BF16), up, pieces)
    high, low = split(pair[1:2])
    mask = up == lax.broadcasted_iota(jnp.int32, (pieces, up.shape[1]), 0)
    last = jnp.concatenate([jnp.where(mask, high, 0.0), jnp.where(mask, low, 0.0)], axis=0).astype(BF16)
    lhs = jnp.concatenate(tiles + [last], axis=0)
    acc[...] += lax.dot_general(lhs, one_hot, DIMS, preferred_element_type=F32)


def add_block(most, two, ids, one_hot, terms, acc):
    pieces, _, width = acc.shape
    lead, trail = most[0:9], jnp.concatenate([most[9:16], two], axis=0)
    at = 0
    for k in range(9):
        terms[at : at + 9 - k, :] = lead[k : k + 1] * lead[k:9] + trail[k : k + 1] * trail[k:9]
        at += 9 - k
    high, low = split(terms[...])
    both = jnp.concatenate([high, low], axis=0).astype(BF16)
    up, _ = place_of(ids, width)
    lhs = jnp.concatenate(masked_tiles(both, up, pieces), axis=0)
    added = lax.dot_general(lhs, one_hot, DIMS, preferred_element_type=F32)
    for h in range(pieces):
        at = h * 2 * KEPT
        acc[h] += added[at : at + KEPT] + added[at + KEPT : at + 2 * KEPT]


def expand(blocks, out):
    m, _, width = blocks.shape
    at = 0
    for k in range(9):
        for l in range(k, 9):
            for r in range(m):
                row = blocks[r, at : at + 1, :]
                lanes = slice(r * width, (r + 1) * width)
                out[k * 9 + l : k * 9 + l + 1, lanes] = row
                if l != k:
                    out[l * 9 + k : l * 9 + k + 1, lanes] = row
            at += 1


def side_ids(o, side, pieces, cmap, width):
    m = PAIR * pieces

    def at(j):
        return pl.ds(pl.multiple_of((o * m + side + PAIR * j) * width, width), width)

    return jnp.concatenate([cmap[:, at(j)] for j in range(pieces)], axis=1)


def place_chunk(eight, ninth, ids, one_hot, acc):
    span = ids.shape[1]
    highs = acc.shape[0] // 18
    up = ids // LOW
    if one_hot is None:
        one_hot = one_hot_of(lax.rem(ids, LOW), LOW)
    high, low = split(eight)
    top = jnp.concatenate([high, low], axis=0).astype(BF16)
    up16 = jnp.broadcast_to(up.astype(F32), (16, span)).astype(BF16)
    none = jnp.zeros_like(top)
    mask = up == lax.broadcasted_iota(jnp.int32, (highs, span), 0)
    high, low = split(ninth)
    last = jnp.concatenate([jnp.where(mask, high, 0.0), jnp.where(mask, low, 0.0)], axis=0).astype(BF16)
    group = min(highs, 32)

    def tiles(start):
        return [jnp.where(up16 == jnp.asarray(start + h, F32).astype(BF16), top, none) for h in range(group)]

    if group == highs:
        lhs = jnp.concatenate(tiles(0) + [last], axis=0)
        acc[...] += lax.dot_general(lhs, one_hot, DIMS, preferred_element_type=F32)
        return

    def some(g, carry):
        lhs = jnp.concatenate(tiles(g * group), axis=0)
        where = pl.ds(pl.multiple_of(g * group * 16, group * 16), group * 16)
        acc[where, :] += lax.dot_general(lhs, one_hot, DIMS, preferred_element_type=F32)
        return carry

    lax.fori_loop(0, highs // group, some, 0)
    acc[highs * 16 :, :] += lax.dot_general(last, one_hot, DIMS, preferred_element_type=F32)


def lay_out(acc, out8, out9, first, last):
    highs = out8.shape[1] // LOW
    for h in range(first, last):
        lanes = slice(h * LOW, (h + 1) * LOW)
        out8[:, lanes] = acc[h * 16 : h * 16 + 8, :] + acc[h * 16 + 8 : h * 16 + 16, :]
        ninth = highs * 16 + h
        out9[:, lanes] = acc[ninth : ninth + 1, :] + acc[ninth + highs : ninth + highs + 1, :]


def main_kernel(
    n, m, counts, jac_in, res_in, ids_in, cmap_in, gradient, out, jac, res, ids, cmap, load_sem,
    tail, own4, own2, own8, got16, got4, got2, got8, late16, late2, hots, terms, gsum, part, fold, landed, total, blocks,
    part8, part9, land8, land9, mine8, mine9, grads8, grads9, ready, spread, out8, out9, sib8, sib9,
    x_send, x_recv, a_send, a_recv, g_send, g_recv, c_send, c_recv, b_send, b_recv, w_send, w_recv, d_send, d_recv,
):
    me, rep = lax.axis_index("obs"), lax.axis_index("rep")
    width = total.shape[2]
    cap, cut = got2.shape[2], got16.shape[2]
    half = m // PAIR
    sibling = rep + 1 - 2 * lax.rem(rep, PAIR)
    barrier = pltpu.get_barrier_semaphore()

    flip = flipper(me, n)

    def greet(i):
        pl.semaphore_signal(barrier, inc=1, device_id={"obs": flip(i)}, device_id_type=MESH)

    each(1, n, greet)
    for i in range(1, m):
        pl.semaphore_signal(barrier, inc=1, device_id={"rep": lax.rem(rep + i, m)}, device_id_type=MESH)
    pairs = ((jac_in, jac), (res_in, res), (ids_in, ids), (cmap_in, cmap))
    loads = [pltpu.make_async_copy(src, dst, load_sem.at[k]) for k, (src, dst) in enumerate(pairs)]
    for load in loads:
        load.start()
    part[...] = jnp.zeros_like(part)
    terms[...] = jnp.zeros_like(terms)
    gsum[...] = jnp.zeros_like(gsum)
    spread[...] = jnp.zeros_like(spread)
    for load in loads:
        load.wait()
    pack(counts, jac, res, ids, tail, own4, own2, own8)
    pl.semaphore_wait(barrier, n + m - 2)

    def lanes_of(peer, first, count):
        return pl.ds(pl.multiple_of(peer * cap + first, 128), count)

    def handing(i, kinds):
        peer = flip(i)
        low, high = lanes_of(peer, 0, cut), lanes_of(peer, cut, cap - cut)
        sent = (
            own2.at[:, lanes_of(peer, 0, cap)], jac.at[0:16, low], own4.at[:, low], own8.at[:, high],
            jac.at[0:16, high], tail.at[:, high],
        )
        taken = (got2.at[i], got16.at[i], got4.at[i], got8.at[i], late16.at[i], late2.at[i])
        return [
            pltpu.make_async_remote_copy(
                src_ref=sent[k], dst_ref=taken[k], send_sem=x_send.at[k, i], recv_sem=x_recv.at[k, i],
                device_id={"obs": peer}, device_id_type=MESH,
            )
            for k in kinds
        ]

    def start(kinds):
        def one(i):
            for copy in handing(n - i, kinds):
                copy.start()

        each(1, n, one)

    start((0,))
    start((1, 2, 3))
    early = ready.shape[0] == n
    side = lax.rem(rep, PAIR)

    def hot_at(i):
        return hots.at[i if early else 0]

    def prepare(o, carry):
        ready[o] = one_hot_of(lax.rem(side_ids(o, side, half, cmap, width), LOW), LOW)
        return carry

    def see(i):
        hot_at(i)[...] = one_hot_of(place_of(got2[i, 0:1], width)[1], width)

    def foresee(i, carry):
        for copy in handing(i, (0,)):
            copy.wait_recv()
        if early:
            see(i)
        return carry

    def gradient_of(i):
        most, four = got16[i], got4[i]
        trail = jnp.concatenate([most[9:16], four[0:2]], axis=0)
        near = most[0:9] * four[2:3] + trail * four[3:4]
        eight = jnp.concatenate([near[0:8], got8[i]], axis=1)
        ninth = jnp.concatenate([near[8:9], got2[i, 1:2, cut:]], axis=1)
        add_gradient(eight, jnp.concatenate([got2[i, 0:1], ninth], axis=0), hot_at(i)[...], gsum, m)

    def low_block(i):
        if not early:
            see(i)
        add_block(got16[i], got4[i, 0:2], got2[i, 0:1, 0:cut], hot_at(i)[:, 0:cut], terms.at[:, 0:cut], part)

    def take(i, carry):
        for copy in handing(i, (1, 2, 3)):
            copy.wait_recv()
        if not early:
            see(i)
        gradient_of(i)
        return carry

    def take_both(i, carry):
        take(i, carry)
        low_block(i)
        return carry

    def take_low(i, carry):
        low_block(i)
        return carry

    def take_late(i, carry):
        for copy in handing(i, (4, 5)):
            copy.wait_recv()
        if not early:
            see(i)
        add_block(late16[i], late2[i], got2[i, 0:1, cut:], hot_at(i)[:, cut:], terms.at[:, 0 : cap - cut], part)
        return carry

    mylanes = lanes_of(me, 0, cap)
    hot_at(0)[...] = one_hot_of(place_of(own2[0:1, mylanes], width)[1], width)
    add_gradient(own8[:, mylanes], own2[:, mylanes], hot_at(0)[...], gsum, m)
    add_block(jac[0:16, mylanes], tail[:, mylanes], own2[0:1, mylanes], hot_at(0)[...], terms, part)
    lax.fori_loop(1, n, foresee, 0)
    if early:
        lax.fori_loop(0, n, prepare, 0)
    inline = min(INLINE, n)
    lax.fori_loop(1, inline, take_both, 0)
    lax.fori_loop(inline, n, take, 0)
    for h in range(m):
        part8[h] = gsum[h * 16 : h * 16 + 8, :] + gsum[h * 16 + 8 : h * 16 + 16, :]
        ninth = m * 16 + h
        part9[h] = gsum[ninth : ninth + 1, :] + gsum[ninth + m : ninth + m + 1, :]

    def to_rep(src, dst, s, r, peer):
        return pltpu.make_async_remote_copy(
            src_ref=src, dst_ref=dst, send_sem=s, recv_sem=r, device_id={"rep": peer}, device_id_type=MESH
        )

    heads = []
    for i in range(1, m):
        peer = lax.rem(rep + i, m)
        heads.append(to_rep(part8.at[peer], land8.at[i], a_send.at[0, i], a_recv.at[0, i], peer))
        heads.append(to_rep(part9.at[peer], land9.at[i], a_send.at[1, i], a_recv.at[1, i], peer))
    for copy in heads:
        copy.start()
    start((4, 5))
    lax.fori_loop(inline, n, take_low, 0)
    lax.fori_loop(1, min(EARLY, n), take_late, 0)
    for copy in heads:
        copy.wait_recv()
    eight, ninth = part8[rep], part9[rep]
    for i in range(1, m):
        eight = eight + land8[i]
        ninth = ninth + land9[i]
    mine8[...] = eight
    mine9[...] = ninth
    grads8[lax.div(rep, PAIR), me] = eight
    grads9[lax.div(rep, PAIR), me] = ninth

    def at_origin(origin, source):
        return grads8.at[origin, source], grads9.at[origin, source]

    def reach(i, j):
        where = {"obs": flip(i), "rep": lax.rem(rep + PAIR * j, m)}
        return [
            pltpu.make_async_remote_copy(
                src_ref=src, dst_ref=dst, send_sem=g_send.at[k, i, j], recv_sem=g_recv.at[k, i, j],
                device_id=where, device_id_type=MESH,
            )
            for k, (src, dst) in enumerate(zip((mine8, mine9), at_origin(lax.div(rep, PAIR), me)))
        ]

    def spread_out(i):
        for j in reversed(range(half)):
            for copy in reach(n - i, j):
                copy.start()

    each(1, n, spread_out)
    for j in range(1, half):
        for copy in reach(0, j):
            copy.start()

    def place(i, first):
        source = flip(i)
        for j in range(first, half):
            for copy in reach(i, j):
                copy.wait_recv()
        eight = jnp.concatenate([grads8[j, source] for j in range(half)], axis=1)
        ninth = jnp.concatenate([grads9[j, source] for j in range(half)], axis=1)
        here = side_ids(source, side, half, cmap, width)
        place_chunk(eight, ninth, here, ready[source] if early else None, spread)

    def settle(i, carry):
        place(i, 0)
        return carry

    lax.fori_loop(min(EARLY, n), n, take_late, 0)
    mine_at, other_at = side * half, (1 - side) * half
    folds, wide, back = [], [], []
    for h in range(half):
        folds.append(to_rep(part.at[other_at + h], fold.at[h], b_send.at[h], b_recv.at[h], sibling))
        for j in range(1, half):
            peer = lax.rem(rep + PAIR * j, m)
            wide.append(to_rep(total.at[h], landed.at[j, h], w_send.at[j, h], w_recv.at[j, h], peer))
        back.append(to_rep(blocks.at[mine_at + h], blocks.at[mine_at + h], d_send.at[h], d_recv.at[h], sibling))
    for copy in folds:
        copy.start()
    for h in range(half):
        folds[h].wait_recv()
        total[h] = part[mine_at + h] + fold[h]
        for copy in wide[h * (half - 1) : (h + 1) * (half - 1)]:
            copy.start()
    place(0, 1)
    lax.fori_loop(1, n, settle, 0)
    swaps = []
    highs, step = gradient.shape[1] // LOW, gradient.shape[1] // CUTS
    for c in range(CUTS):
        lanes = pl.ds(c * step, step)
        lay_out(spread, out8, out9, c * highs // CUTS, (c + 1) * highs // CUTS)
        swaps.append(to_rep(out8.at[:, lanes], sib8.at[:, lanes], c_send.at[0, c], c_recv.at[0, c], sibling))
        swaps.append(to_rep(out9.at[:, lanes], sib9.at[:, lanes], c_send.at[1, c], c_recv.at[1, c], sibling))
        for copy in swaps[-2:]:
            copy.start()
    for h in range(half):
        for copy in wide[h * (half - 1) : (h + 1) * (half - 1)]:
            copy.wait_recv()
        full = total[h]
        for j in range(1, half):
            full = full + landed[j, h]
        blocks[mine_at + h] = full
        back[h].start()
    for c in range(CUTS):
        lanes = slice(c * step, (c + 1) * step)
        for copy in swaps[2 * c : 2 * c + 2]:
            copy.wait_recv()
        gradient[0:8, lanes] = out8[:, lanes] + sib8[:, lanes]
        gradient[8:9, lanes] = out9[:, lanes] + sib9[:, lanes]
    for copy in back:
        copy.wait_recv()
    expand(blocks, out)

    def finish(i):
        for copy in handing(i, (0, 1, 2, 3, 4, 5)):
            copy.wait_send()
        for j in range(half):
            for copy in reach(i, j):
                copy.wait_send()

    each(1, n, finish)
    for j in range(1, half):
        for copy in reach(0, j):
            copy.wait_send()
    for copy in heads + folds + wide + back + swaps:
        copy.wait_send()


def write_kernel(gradient, blocks, gradient_out, blocks_out, out_sem):
    def cut(ref, count):
        step = ref.shape[1] // count
        return [ref.at[:, pl.ds(c * step, step)] for c in range(count)]

    jobs = list(zip(cut(blocks, 2), cut(blocks_out, 2)))
    jobs += list(zip(cut(gradient, 4), cut(gradient_out, 4)))
    writes = [pltpu.make_async_copy(job[0], job[1], out_sem.at[j]) for j, job in enumerate(jobs)]
    for write in writes:
        write.start()
    for write in writes:
        write.wait()


def local(jacobians, residuals, camera_local, bucket_counts, camera_map):
    n, m = lax.axis_size("obs"), lax.axis_size("rep")
    slots = jacobians.shape[1]
    cap = slots // n
    cut = cap // 2
    cams = camera_map.shape[0]
    width = CAM_DEV // m
    highs = cams // LOW
    half = m // PAIR
    dma = pltpu.SemaphoreType.DMA
    early = n * LOW * CAM_DEV * 2 <= 8 * MIB
    kept = n if early else 1
    held = 16 * cams * 4 + 88 * CAM_DEV * 4
    limit = 60 * MIB - max(0, held - 2 * MIB)
    gradient, out = pl.pallas_call(
        functools.partial(main_kernel, n, m),
        out_shape=(VMEM((9, cams), F32), VMEM((81, CAM_DEV), F32)),
        in_specs=[pl.BlockSpec(memory_space=pltpu.SMEM)] + [pl.BlockSpec(memory_space=pltpu.HBM)] * 4,
        out_specs=(vspec(), vspec()),
        scratch_shapes=[
            VMEM((18, slots), F32),
            VMEM((2, slots), F32),
            VMEM((1, slots), jnp.int32),
            VMEM((1, cams), jnp.int32),
            dma((4,)),
            VMEM((2, slots), F32),
            VMEM((4, slots), F32),
            VMEM((2, slots), F32),
            VMEM((8, slots), F32),
            VMEM((n, 16, cut), F32),
            VMEM((n, 4, cut), F32),
            VMEM((n, 2, cap), F32),
            VMEM((n, 8, cap - cut), F32),
            VMEM((n, 16, cap - cut), F32),
            VMEM((n, 2, cap - cut), F32),
            VMEM((kept, width, cap), BF16),
            VMEM((KEPT, cap), F32),
            VMEM((m * 18, width), F32),
            VMEM((m, KEPT, width), F32),
            VMEM((half, KEPT, width), F32),
            VMEM((half, half, KEPT, width), F32),
            VMEM((half, KEPT, width), F32),
            VMEM((m, KEPT, width), F32),
            VMEM((m, 8, width), F32),
            VMEM((m, 1, width), F32),
            VMEM((m, 8, width), F32),
            VMEM((m, 1, width), F32),
            VMEM((8, width), F32),
            VMEM((1, width), F32),
            VMEM((half, n, 8, width), F32),
            VMEM((half, n, 1, width), F32),
            VMEM((kept, LOW, half * width), BF16),
            VMEM((highs * 18, LOW), F32),
            VMEM((8, cams), F32),
            VMEM((1, cams), F32),
            VMEM((8, cams), F32),
            VMEM((1, cams), F32),
            dma((6, n)),
            dma((6, n)),
            dma((2, m)),
            dma((2, m)),
            dma((2, n, half)),
            dma((2, n, half)),
            dma((2, CUTS)),
            dma((2, CUTS)),
            dma((half,)),
            dma((half,)),
            dma((half, half)),
            dma((half, half)),
            dma((half,)),
            dma((half,)),
        ],
        compiler_params=pltpu.CompilerParams(collective_id=0, has_side_effects=True, vmem_limit_bytes=limit),
    )(bucket_counts, jacobians, residuals, camera_local.reshape(1, slots), camera_map.reshape(1, cams))
    anywhere = pl.BlockSpec(memory_space=pl.ANY)
    shapes = (jax.ShapeDtypeStruct(gradient.shape, F32), jax.ShapeDtypeStruct(out.shape, F32))
    return pl.pallas_call(
        write_kernel,
        out_shape=shapes,
        in_specs=[vspec()] * 2,
        out_specs=(anywhere, anywhere),
        scratch_shapes=[dma((6,))],
        compiler_params=pltpu.CompilerParams(vmem_limit_bytes=2 * MIB),
    )(gradient, out)


def solution(mesh):
    in_specs = (
        P(None, ("obs", "rep")),
        P(None, ("obs", "rep")),
        P(("obs", "rep")),
        P(("obs", "rep"), None),
        P(),
    )
    out_specs = (P(), P(None, "obs"))
    return jax.shard_map(local, mesh=mesh, in_specs=in_specs, out_specs=out_specs, check_vma=False)
```

```python
import functools

import jax
import jax.numpy as jnp
from jax import lax
from jax.experimental import pallas as pl
from jax.experimental.pallas import tpu as pltpu
from jax.sharding import PartitionSpec as P

CAM_DEV = 1024
MESH = pl.DeviceIdType.MESH
F32 = jnp.float32
BF16 = jnp.bfloat16
VMEM = pltpu.VMEM
KEPT = 48
CUTS = 2
EARLY = 1
INLINE = 1
LOW = 256
PAIR = 2
MIB = 1024 * 1024
DIMS = (((1,), (1,)), ((), ()))


def vspec():
    return pl.BlockSpec(memory_space=VMEM)


def flipper(me, size):
    weights = [1 << k for k in range(size.bit_length() - 1)]
    signed = [w * (1 - 2 * lax.rem(me // w, 2)) for w in weights]

    def flip(i):
        out = me
        for w, s in zip(weights, signed):
            if isinstance(i, int):
                out = out + s if i // w % 2 else out
            else:
                out = out + s * lax.rem(lax.div(i, w), 2)
        return out

    return flip


def each(first, last, body):
    if last - first <= 8:
        for i in range(first, last):
            body(i)
    else:
        lax.fori_loop(first, last, lambda i, carry: (body(i), carry)[1], 0)


def split(value):
    high = value.astype(BF16).astype(F32)
    return high, value - high


def pack(counts, jac, res, ids, tail, own4, own2, own8):
    buckets = counts.shape[1]
    cap = jac.shape[1] // buckets
    tail[...] = jac[16:18, :]
    own4[0:2, :] = jac[16:18, :]
    own4[2:4, :] = res[...]
    own8[...] = jac[0:8, :] * res[0:1, :] + jac[9:17, :] * res[1:2, :]
    own2[1:2, :] = jac[8:9, :] * res[0:1, :] + jac[17:18, :] * res[1:2, :]
    place = lax.broadcasted_iota(jnp.int32, (1, cap), 1)
    for d in range(buckets):
        lanes = slice(d * cap, (d + 1) * cap)
        own2[0:1, lanes] = jnp.where(place < counts[0, d], ids[:, lanes], -1).astype(F32)


def one_hot_of(low, wide):
    shape = (wide, low.shape[1])
    rows = lax.broadcasted_iota(jnp.int32, shape, 0).astype(F32).astype(BF16)
    there = jnp.broadcast_to(low.astype(F32), shape).astype(BF16)
    return jnp.where(there == rows, jnp.ones(shape, BF16), jnp.zeros(shape, BF16))


def place_of(ids, width):
    ids = ids.astype(jnp.int32)
    up = jnp.where(ids < 0, -1, ids // width)
    return up, ids - up * width


def masked_tiles(value, up, pieces):
    up = jnp.broadcast_to(up.astype(F32), value.shape).astype(BF16)
    zero = jnp.zeros_like(value)
    return [jnp.where(up == jnp.asarray(h, BF16), value, zero) for h in range(pieces)]


def add_gradient(eight, pair, one_hot, acc, pieces):
    up, _ = place_of(pair[0:1], acc.shape[1])
    high, low = split(eight)
    tiles = masked_tiles(jnp.concatenate([high, low], axis=0).astype(BF16), up, pieces)
    high, low = split(pair[1:2])
    mask = up == lax.broadcasted_iota(jnp.int32, (pieces, up.shape[1]), 0)
    last = jnp.concatenate([jnp.where(mask, high, 0.0), jnp.where(mask, low, 0.0)], axis=0).astype(BF16)
    lhs = jnp.concatenate(tiles + [last], axis=0)
    acc[...] += lax.dot_general(lhs, one_hot, DIMS, preferred_element_type=F32)


def add_block(most, two, ids, one_hot, terms, acc):
    pieces, _, width = acc.shape
    lead, trail = most[0:9], jnp.concatenate([most[9:16], two], axis=0)
    at = 0
    for k in range(9):
        terms[at : at + 9 - k, :] = lead[k : k + 1] * lead[k:9] + trail[k : k + 1] * trail[k:9]
        at += 9 - k
    high, low = split(terms[...])
    both = jnp.concatenate([high, low], axis=0).astype(BF16)
    up, _ = place_of(ids, width)
    lhs = jnp.concatenate(masked_tiles(both, up, pieces), axis=0)
    added = lax.dot_general(lhs, one_hot, DIMS, preferred_element_type=F32)
    for h in range(pieces):
        at = h * 2 * KEPT
        acc[h] += added[at : at + KEPT] + added[at + KEPT : at + 2 * KEPT]


def expand(blocks, out):
    m, _, width = blocks.shape
    at = 0
    for k in range(9):
        for l in range(k, 9):
            for r in range(m):
                row = blocks[r, at : at + 1, :]
                lanes = slice(r * width, (r + 1) * width)
                out[k * 9 + l : k * 9 + l + 1, lanes] = row
                if l != k:
                    out[l * 9 + k : l * 9 + k + 1, lanes] = row
            at += 1


def side_ids(o, side, pieces, cmap, width):
    m = PAIR * pieces

    def at(j):
        return pl.ds(pl.multiple_of((o * m + side + PAIR * j) * width, width), width)

    return jnp.concatenate([cmap[:, at(j)] for j in range(pieces)], axis=1)


def place_chunk(eight, ninth, ids, one_hot, acc):
    span = ids.shape[1]
    highs = acc.shape[0] // 18
    up = ids // LOW
    if one_hot is None:
        one_hot = one_hot_of(lax.rem(ids, LOW), LOW)
    high, low = split(eight)
    top = jnp.concatenate([high, low], axis=0).astype(BF16)
    up16 = jnp.broadcast_to(up.astype(F32), (16, span)).astype(BF16)
    none = jnp.zeros_like(top)
    mask = up == lax.broadcasted_iota(jnp.int32, (highs, span), 0)
    high, low = split(ninth)
    last = jnp.concatenate([jnp.where(mask, high, 0.0), jnp.where(mask, low, 0.0)], axis=0).astype(BF16)
    group = min(highs, 32)

    def tiles(start):
        return [jnp.where(up16 == jnp.asarray(start + h, F32).astype(BF16), top, none) for h in range(group)]

    if group == highs:
        lhs = jnp.concatenate(tiles(0) + [last], axis=0)
        acc[...] += lax.dot_general(lhs, one_hot, DIMS, preferred_element_type=F32)
        return

    def some(g, carry):
        lhs = jnp.concatenate(tiles(g * group), axis=0)
        where = pl.ds(pl.multiple_of(g * group * 16, group * 16), group * 16)
        acc[where, :] += lax.dot_general(lhs, one_hot, DIMS, preferred_element_type=F32)
        return carry

    lax.fori_loop(0, highs // group, some, 0)
    acc[highs * 16 :, :] += lax.dot_general(last, one_hot, DIMS, preferred_element_type=F32)


def lay_out(acc, out8, out9, first, last):
    highs = out8.shape[1] // LOW
    for h in range(first, last):
        lanes = slice(h * LOW, (h + 1) * LOW)
        out8[:, lanes] = acc[h * 16 : h * 16 + 8, :] + acc[h * 16 + 8 : h * 16 + 16, :]
        ninth = highs * 16 + h
        out9[:, lanes] = acc[ninth : ninth + 1, :] + acc[ninth + highs : ninth + highs + 1, :]


def main_kernel(
    n, m, counts, jac_in, res_in, ids_in, cmap_in, gradient, out, jac, res, ids, cmap, load_sem,
    tail, own4, own2, own8, got16, got4, got2, got8, late16, late2, hots, terms, gsum, part, fold, landed, total, blocks,
    part8, part9, land8, land9, mine, grads, ready, spread, out8, out9, sib8, sib9,
    x_send, x_recv, a_send, a_recv, g_send, g_recv, c_send, c_recv, b_send, b_recv, w_send, w_recv, d_send, d_recv,
):
    me, rep = lax.axis_index("obs"), lax.axis_index("rep")
    width = total.shape[2]
    cap, cut = got2.shape[2], got16.shape[2]
    half = m // PAIR
    sibling = rep + 1 - 2 * lax.rem(rep, PAIR)
    barrier = pltpu.get_barrier_semaphore()

    flip = flipper(me, n)

    def greet(i):
        pl.semaphore_signal(barrier, inc=1, device_id={"obs": flip(i)}, device_id_type=MESH)

    each(1, n, lambda i: greet(n - i))
    for i in range(1, m):
        pl.semaphore_signal(barrier, inc=1, device_id={"rep": lax.rem(rep + i, m)}, device_id_type=MESH)
    pairs = ((jac_in, jac), (res_in, res), (ids_in, ids), (cmap_in, cmap))
    loads = [pltpu.make_async_copy(src, dst, load_sem.at[k]) for k, (src, dst) in enumerate(pairs)]
    for load in loads:
        load.start()
    part[...] = jnp.zeros_like(part)
    terms[...] = jnp.zeros_like(terms)
    gsum[...] = jnp.zeros_like(gsum)
    spread[...] = jnp.zeros_like(spread)
    for load in loads:
        load.wait()
    pack(counts, jac, res, ids, tail, own4, own2, own8)
    pl.semaphore_wait(barrier, n + m - 2)

    def lanes_of(peer, first, count):
        return pl.ds(pl.multiple_of(peer * cap + first, 128), count)

    def handing(i, kinds):
        peer = flip(i)
        low, high = lanes_of(peer, 0, cut), lanes_of(peer, cut, cap - cut)
        sent = (
            own2.at[:, lanes_of(peer, 0, cap)], jac.at[0:16, low], own4.at[:, low], own8.at[:, high],
            jac.at[0:16, high], tail.at[:, high],
        )
        taken = (got2.at[i], got16.at[i], got4.at[i], got8.at[i], late16.at[i], late2.at[i])
        return [
            pltpu.make_async_remote_copy(
                src_ref=sent[k], dst_ref=taken[k], send_sem=x_send.at[k, i], recv_sem=x_recv.at[k, i],
                device_id={"obs": peer}, device_id_type=MESH,
            )
            for k in kinds
        ]

    def start(kinds, first, last):
        def one(i):
            for copy in handing(first + last - 1 - i, kinds):
                copy.start()

        each(first, last, one)

    start((0,), 1, n)
    start((1, 2, 3), 2, n)
    start((1, 2, 3, 4, 5), 1, 2)
    early = ready.shape[0] == n
    side = lax.rem(rep, PAIR)

    def hot_at(i):
        return hots.at[i if early else 0]

    def prepare(o, carry):
        ready[o] = one_hot_of(lax.rem(side_ids(o, side, half, cmap, width), LOW), LOW)
        return carry

    def see(i):
        hot_at(i)[...] = one_hot_of(place_of(got2[i, 0:1], width)[1], width)

    def foresee(i, carry):
        for copy in handing(i, (0,)):
            copy.wait_recv()
        if early:
            see(i)
        return carry

    def gradient_of(i):
        most, four = got16[i], got4[i]
        trail = jnp.concatenate([most[9:16], four[0:2]], axis=0)
        near = most[0:9] * four[2:3] + trail * four[3:4]
        eight = jnp.concatenate([near[0:8], got8[i]], axis=1)
        ninth = jnp.concatenate([near[8:9], got2[i, 1:2, cut:]], axis=1)
        add_gradient(eight, jnp.concatenate([got2[i, 0:1], ninth], axis=0), hot_at(i)[...], gsum, m)

    def low_block(i):
        if not early:
            see(i)
        add_block(got16[i], got4[i, 0:2], got2[i, 0:1, 0:cut], hot_at(i)[:, 0:cut], terms.at[:, 0:cut], part)

    def take(i, carry):
        for copy in handing(i, (1, 2, 3)):
            copy.wait_recv()
        if not early:
            see(i)
        gradient_of(i)
        return carry

    def take_both(i, carry):
        take(i, carry)
        low_block(i)
        return carry

    def take_low(i, carry):
        low_block(i)
        return carry

    def take_late(i, carry):
        for copy in handing(i, (4, 5)):
            copy.wait_recv()
        if not early:
            see(i)
        add_block(late16[i], late2[i], got2[i, 0:1, cut:], hot_at(i)[:, cut:], terms.at[:, 0 : cap - cut], part)
        return carry

    mylanes = lanes_of(me, 0, cap)
    hot_at(0)[...] = one_hot_of(place_of(own2[0:1, mylanes], width)[1], width)
    add_gradient(own8[:, mylanes], own2[:, mylanes], hot_at(0)[...], gsum, m)
    add_block(jac[0:16, mylanes], tail[:, mylanes], own2[0:1, mylanes], hot_at(0)[...], terms, part)
    lax.fori_loop(1, n, foresee, 0)
    if early:
        lax.fori_loop(0, n, prepare, 0)
    inline = min(INLINE, n)
    lax.fori_loop(1, inline, take_both, 0)
    lax.fori_loop(inline, n, take, 0)
    for h in range(m):
        part8[h] = gsum[h * 16 : h * 16 + 8, :] + gsum[h * 16 + 8 : h * 16 + 16, :]
        ninth = m * 16 + h
        part9[h] = gsum[ninth : ninth + 1, :] + gsum[ninth + m : ninth + m + 1, :]

    def to_rep(src, dst, s, r, peer):
        return pltpu.make_async_remote_copy(
            src_ref=src, dst_ref=dst, send_sem=s, recv_sem=r, device_id={"rep": peer}, device_id_type=MESH
        )

    heads = []
    for i in range(1, m):
        peer = lax.rem(rep + i, m)
        heads.append(to_rep(part8.at[peer], land8.at[i], a_send.at[0, i], a_recv.at[0, i], peer))
        heads.append(to_rep(part9.at[peer], land9.at[i], a_send.at[1, i], a_recv.at[1, i], peer))
    for copy in heads:
        copy.start()
    start((4, 5), 2, n)
    lax.fori_loop(inline, n, take_low, 0)
    lax.fori_loop(1, min(EARLY, n), take_late, 0)
    for copy in heads:
        copy.wait_recv()
    eight, ninth = part8[rep], part9[rep]
    for i in range(1, m):
        eight = eight + land8[i]
        ninth = ninth + land9[i]
    for k in range(9):
        row = eight[k : k + 1] if k < 8 else ninth
        mine[k] = row
        grads[lax.div(rep, PAIR), me, k] = row

    def reach(i, j):
        where = {"obs": flip(i), "rep": lax.rem(rep + PAIR * j, m)}
        return [
            pltpu.make_async_remote_copy(
                src_ref=mine, dst_ref=grads.at[lax.div(rep, PAIR), me], send_sem=g_send.at[i, j],
                recv_sem=g_recv.at[i, j], device_id=where, device_id_type=MESH,
            )
        ]

    def spread_out(i):
        for j in reversed(range(half)):
            for copy in reach(n - i, j):
                copy.start()

    each(1, n, spread_out)
    for j in range(1, half):
        for copy in reach(0, j):
            copy.start()

    def place(i, first):
        source = flip(i)
        for j in range(first, half):
            for copy in reach(i, j):
                copy.wait_recv()
        rows = [jnp.concatenate([grads[j, source, k] for j in range(half)], axis=1) for k in range(9)]
        eight, ninth = jnp.concatenate(rows[0:8], axis=0), rows[8]
        here = side_ids(source, side, half, cmap, width)
        place_chunk(eight, ninth, here, ready[source] if early else None, spread)

    def settle(i, carry):
        place(i, 0)
        return carry

    lax.fori_loop(min(EARLY, n), n, take_late, 0)
    mine_at, other_at = side * half, (1 - side) * half
    folds, wide, back = [], [], []
    for h in range(half):
        folds.append(to_rep(part.at[other_at + h], fold.at[h], b_send.at[h], b_recv.at[h], sibling))
        for j in range(1, half):
            peer = lax.rem(rep + PAIR * j, m)
            wide.append(to_rep(total.at[h], landed.at[j, h], w_send.at[j, h], w_recv.at[j, h], peer))
        back.append(to_rep(blocks.at[mine_at + h], blocks.at[mine_at + h], d_send.at[h], d_recv.at[h], sibling))
    for copy in folds:
        copy.start()
    for h in range(half):
        folds[h].wait_recv()
        total[h] = part[mine_at + h] + fold[h]
        for copy in wide[h * (half - 1) : (h + 1) * (half - 1)]:
            copy.start()
    def drain(i):
        for copy in handing(i, (0, 1, 2, 3, 4, 5)):
            copy.wait_send()

    def drain_reach(i):
        for j in range(half):
            for copy in reach(i, j):
                copy.wait_send()

    each(1, n, drain)
    for copy in heads + folds:
        copy.wait_send()
    place(0, 1)
    lax.fori_loop(1, n, settle, 0)
    swaps = []
    highs, step = gradient.shape[1] // LOW, gradient.shape[1] // CUTS
    for c in range(CUTS):
        lanes = pl.ds(c * step, step)
        lay_out(spread, out8, out9, c * highs // CUTS, (c + 1) * highs // CUTS)
        swaps.append(to_rep(out8.at[:, lanes], sib8.at[:, lanes], c_send.at[0, c], c_recv.at[0, c], sibling))
        swaps.append(to_rep(out9.at[:, lanes], sib9.at[:, lanes], c_send.at[1, c], c_recv.at[1, c], sibling))
        for copy in swaps[-2:]:
            copy.start()
    each(1, n, drain_reach)
    for j in range(1, half):
        for copy in reach(0, j):
            copy.wait_send()
    for h in range(half):
        for copy in wide[h * (half - 1) : (h + 1) * (half - 1)]:
            copy.wait_recv()
        full = total[h]
        for j in range(1, half):
            full = full + landed[j, h]
        blocks[mine_at + h] = full
        back[h].start()
    for copy in wide:
        copy.wait_send()
    for c in range(CUTS):
        lanes = slice(c * step, (c + 1) * step)
        for copy in swaps[2 * c : 2 * c + 2]:
            copy.wait_recv()
        gradient[0:8, lanes] = out8[:, lanes] + sib8[:, lanes]
        gradient[8:9, lanes] = out9[:, lanes] + sib9[:, lanes]
    for copy in back:
        copy.wait_recv()
    expand(blocks, out)

    for copy in back + swaps:
        copy.wait_send()


def write_kernel(gradient, blocks, gradient_out, blocks_out, out_sem):
    def cut(ref, count):
        step = ref.shape[1] // count
        return [ref.at[:, pl.ds(c * step, step)] for c in range(count)]

    jobs = list(zip(cut(blocks, 2), cut(blocks_out, 2)))
    jobs += list(zip(cut(gradient, 4), cut(gradient_out, 4)))
    writes = [pltpu.make_async_copy(job[0], job[1], out_sem.at[j]) for j, job in enumerate(jobs)]
    for write in writes:
        write.start()
    for write in writes:
        write.wait()


def local(jacobians, residuals, camera_local, bucket_counts, camera_map):
    n, m = lax.axis_size("obs"), lax.axis_size("rep")
    slots = jacobians.shape[1]
    cap = slots // n
    cut = cap // 2
    cams = camera_map.shape[0]
    width = CAM_DEV // m
    highs = cams // LOW
    half = m // PAIR
    dma = pltpu.SemaphoreType.DMA
    early = n * LOW * CAM_DEV * 2 <= 8 * MIB
    kept = n if early else 1
    held = 16 * cams * 4 + 88 * CAM_DEV * 4
    limit = 60 * MIB - max(0, held - 2 * MIB)
    gradient, out = pl.pallas_call(
        functools.partial(main_kernel, n, m),
        out_shape=(VMEM((9, cams), F32), VMEM((81, CAM_DEV), F32)),
        in_specs=[pl.BlockSpec(memory_space=pltpu.SMEM)] + [pl.BlockSpec(memory_space=pltpu.HBM)] * 4,
        out_specs=(vspec(), vspec()),
        scratch_shapes=[
            VMEM((18, slots), F32),
            VMEM((2, slots), F32),
            VMEM((1, slots), jnp.int32),
            VMEM((1, cams), jnp.int32),
            dma((4,)),
            VMEM((2, slots), F32),
            VMEM((4, slots), F32),
            VMEM((2, slots), F32),
            VMEM((8, slots), F32),
            VMEM((n, 16, cut), F32),
            VMEM((n, 4, cut), F32),
            VMEM((n, 2, cap), F32),
            VMEM((n, 8, cap - cut), F32),
            VMEM((n, 16, cap - cut), F32),
            VMEM((n, 2, cap - cut), F32),
            VMEM((kept, width, cap), BF16),
            VMEM((KEPT, cap), F32),
            VMEM((m * 18, width), F32),
            VMEM((m, KEPT, width), F32),
            VMEM((half, KEPT, width), F32),
            VMEM((half, half, KEPT, width), F32),
            VMEM((half, KEPT, width), F32),
            VMEM((m, KEPT, width), F32),
            VMEM((m, 8, width), F32),
            VMEM((m, 1, width), F32),
            VMEM((m, 8, width), F32),
            VMEM((m, 1, width), F32),
            VMEM((9, 1, width), F32),
            VMEM((half, n, 9, 1, width), F32),
            VMEM((kept, LOW, half * width), BF16),
            VMEM((highs * 18, LOW), F32),
            VMEM((8, cams), F32),
            VMEM((1, cams), F32),
            VMEM((8, cams), F32),
            VMEM((1, cams), F32),
            dma((6, n)),
            dma((6, n)),
            dma((2, m)),
            dma((2, m)),
            dma((n, half)),
            dma((n, half)),
            dma((2, CUTS)),
            dma((2, CUTS)),
            dma((half,)),
            dma((half,)),
            dma((half, half)),
            dma((half, half)),
            dma((half,)),
            dma((half,)),
        ],
        compiler_params=pltpu.CompilerParams(collective_id=0, has_side_effects=True, vmem_limit_bytes=limit),
    )(bucket_counts, jacobians, residuals, camera_local.reshape(1, slots), camera_map.reshape(1, cams))
    anywhere = pl.BlockSpec(memory_space=pl.ANY)
    shapes = (jax.ShapeDtypeStruct(gradient.shape, F32), jax.ShapeDtypeStruct(out.shape, F32))
    return pl.pallas_call(
        write_kernel,
        out_shape=shapes,
        in_specs=[vspec()] * 2,
        out_specs=(anywhere, anywhere),
        scratch_shapes=[dma((6,))],
        compiler_params=pltpu.CompilerParams(vmem_limit_bytes=2 * MIB),
    )(gradient, out)


def solution(mesh):
    in_specs = (
        P(None, ("obs", "rep")),
        P(None, ("obs", "rep")),
        P(("obs", "rep")),
        P(("obs", "rep"), None),
        P(),
    )
    out_specs = (P(), P(None, "obs"))
    return jax.shard_map(local, mesh=mesh, in_specs=in_specs, out_specs=out_specs, check_vma=False)
```

```python
import functools

import jax
import jax.numpy as jnp
from jax import lax
from jax.experimental import pallas as pl
from jax.experimental.pallas import tpu as pltpu
from jax.sharding import PartitionSpec as P

CAM_DEV = 1024
MESH = pl.DeviceIdType.MESH
F32 = jnp.float32
BF16 = jnp.bfloat16
VMEM = pltpu.VMEM
KEPT = 48
CUTS = 1
EARLY = 1
INLINE = 1
LOW = 256
PAIR = 2
MIB = 1024 * 1024
DIMS = (((1,), (1,)), ((), ()))


def vspec():
    return pl.BlockSpec(memory_space=VMEM)


def flipper(me, size):
    weights = [1 << k for k in range(size.bit_length() - 1)]
    signed = [w * (1 - 2 * lax.rem(me // w, 2)) for w in weights]

    def flip(i):
        out = me
        for w, s in zip(weights, signed):
            if isinstance(i, int):
                out = out + s if i // w % 2 else out
            else:
                out = out + s * lax.rem(lax.div(i, w), 2)
        return out

    return flip


def each(first, last, body):
    if last - first <= 8:
        for i in range(first, last):
            body(i)
    else:
        lax.fori_loop(first, last, lambda i, carry: (body(i), carry)[1], 0)


def split(value):
    high = value.astype(BF16).astype(F32)
    return high, value - high


def pack(counts, jac, res, ids, tail, own4, own2, own8):
    buckets = counts.shape[1]
    cap = jac.shape[1] // buckets
    tail[...] = jac[16:18, :]
    own4[0:2, :] = jac[16:18, :]
    own4[2:4, :] = res[...]
    own8[...] = jac[0:8, :] * res[0:1, :] + jac[9:17, :] * res[1:2, :]
    own2[1:2, :] = jac[8:9, :] * res[0:1, :] + jac[17:18, :] * res[1:2, :]
    place = lax.broadcasted_iota(jnp.int32, (1, cap), 1)
    for d in range(buckets):
        lanes = slice(d * cap, (d + 1) * cap)
        own2[0:1, lanes] = jnp.where(place < counts[0, d], ids[:, lanes], -1).astype(F32)


def one_hot_of(low, wide):
    shape = (wide, low.shape[1])
    rows = lax.broadcasted_iota(jnp.int32, shape, 0).astype(F32).astype(BF16)
    there = jnp.broadcast_to(low.astype(F32), shape).astype(BF16)
    return jnp.where(there == rows, jnp.ones(shape, BF16), jnp.zeros(shape, BF16))


def place_of(ids, width):
    ids = ids.astype(jnp.int32)
    up = jnp.where(ids < 0, -1, ids // width)
    return up, ids - up * width


def masked_tiles(value, up, pieces):
    up = jnp.broadcast_to(up.astype(F32), value.shape).astype(BF16)
    zero = jnp.zeros_like(value)
    return [jnp.where(up == jnp.asarray(h, BF16), value, zero) for h in range(pieces)]


def add_gradient(eight, pair, one_hot, acc, pieces):
    up, _ = place_of(pair[0:1], acc.shape[1])
    high, low = split(eight)
    tiles = masked_tiles(jnp.concatenate([high, low], axis=0).astype(BF16), up, pieces)
    high, low = split(pair[1:2])
    mask = up == lax.broadcasted_iota(jnp.int32, (pieces, up.shape[1]), 0)
    last = jnp.concatenate([jnp.where(mask, high, 0.0), jnp.where(mask, low, 0.0)], axis=0).astype(BF16)
    lhs = jnp.concatenate(tiles + [last], axis=0)
    acc[...] += lax.dot_general(lhs, one_hot, DIMS, preferred_element_type=F32)


def add_block(most, two, ids, one_hot, terms, acc):
    pieces, _, width = acc.shape
    lead, trail = most[0:9], jnp.concatenate([most[9:16], two], axis=0)
    at = 0
    for k in range(9):
        terms[at : at + 9 - k, :] = lead[k : k + 1] * lead[k:9] + trail[k : k + 1] * trail[k:9]
        at += 9 - k
    high, low = split(terms[...])
    both = jnp.concatenate([high, low], axis=0).astype(BF16)
    up, _ = place_of(ids, width)
    lhs = jnp.concatenate(masked_tiles(both, up, pieces), axis=0)
    added = lax.dot_general(lhs, one_hot, DIMS, preferred_element_type=F32)
    for h in range(pieces):
        at = h * 2 * KEPT
        acc[h] += added[at : at + KEPT] + added[at + KEPT : at + 2 * KEPT]


def expand(blocks, out):
    m, _, width = blocks.shape
    at = 0
    for k in range(9):
        for l in range(k, 9):
            for r in range(m):
                row = blocks[r, at : at + 1, :]
                lanes = slice(r * width, (r + 1) * width)
                out[k * 9 + l : k * 9 + l + 1, lanes] = row
                if l != k:
                    out[l * 9 + k : l * 9 + k + 1, lanes] = row
            at += 1


def side_ids(o, side, pieces, cmap, width):
    m = PAIR * pieces

    def at(j):
        return pl.ds(pl.multiple_of((o * m + side + PAIR * j) * width, width), width)

    return jnp.concatenate([cmap[:, at(j)] for j in range(pieces)], axis=1)


def place_chunk(eight, ninth, ids, one_hot, acc):
    span = ids.shape[1]
    highs = acc.shape[0] // 18
    up = ids // LOW
    if one_hot is None:
        one_hot = one_hot_of(lax.rem(ids, LOW), LOW)
    high, low = split(eight)
    top = jnp.concatenate([high, low], axis=0).astype(BF16)
    up16 = jnp.broadcast_to(up.astype(F32), (16, span)).astype(BF16)
    none = jnp.zeros_like(top)
    mask = up == lax.broadcasted_iota(jnp.int32, (highs, span), 0)
    high, low = split(ninth)
    last = jnp.concatenate([jnp.where(mask, high, 0.0), jnp.where(mask, low, 0.0)], axis=0).astype(BF16)
    group = min(highs, 32)

    def tiles(start):
        return [jnp.where(up16 == jnp.asarray(start + h, F32).astype(BF16), top, none) for h in range(group)]

    if group == highs:
        lhs = jnp.concatenate(tiles(0) + [last], axis=0)
        acc[...] += lax.dot_general(lhs, one_hot, DIMS, preferred_element_type=F32)
        return

    def some(g, carry):
        lhs = jnp.concatenate(tiles(g * group), axis=0)
        where = pl.ds(pl.multiple_of(g * group * 16, group * 16), group * 16)
        acc[where, :] += lax.dot_general(lhs, one_hot, DIMS, preferred_element_type=F32)
        return carry

    lax.fori_loop(0, highs // group, some, 0)
    acc[highs * 16 :, :] += lax.dot_general(last, one_hot, DIMS, preferred_element_type=F32)


def lay_out(acc, out8, out9, first, last):
    highs = out8.shape[1] // LOW
    for h in range(first, last):
        lanes = slice(h * LOW, (h + 1) * LOW)
        out8[:, lanes] = acc[h * 16 : h * 16 + 8, :] + acc[h * 16 + 8 : h * 16 + 16, :]
        ninth = highs * 16 + h
        out9[:, lanes] = acc[ninth : ninth + 1, :] + acc[ninth + highs : ninth + highs + 1, :]


def main_kernel(
    n, m, counts, jac_in, res_in, ids_in, cmap_in, gradient, out, jac, res, ids, cmap, load_sem,
    tail, own4, own2, own8, got16, got4, got2, got8, late16, late2, hots, terms, gsum, part, fold, landed, total, blocks,
    piece, land, mine, grads, ready, spread, out8, out9, sib8, sib9,
    x_send, x_recv, a_send, a_recv, g_send, g_recv, c_send, c_recv, b_send, b_recv, w_send, w_recv, d_send, d_recv,
):
    me, rep = lax.axis_index("obs"), lax.axis_index("rep")
    width = total.shape[2]
    cap, cut = got2.shape[2], got16.shape[2]
    half = m // PAIR
    sibling = rep + 1 - 2 * lax.rem(rep, PAIR)
    barrier = pltpu.get_barrier_semaphore()

    flip = flipper(me, n)

    def greet(i):
        pl.semaphore_signal(barrier, inc=1, device_id={"obs": flip(i)}, device_id_type=MESH)

    each(1, n, lambda i: greet(n - i))
    for i in range(1, m):
        pl.semaphore_signal(barrier, inc=1, device_id={"rep": lax.rem(rep + i, m)}, device_id_type=MESH)
    pairs = ((jac_in, jac), (res_in, res), (ids_in, ids), (cmap_in, cmap))
    loads = [pltpu.make_async_copy(src, dst, load_sem.at[k]) for k, (src, dst) in enumerate(pairs)]
    for load in loads:
        load.start()
    part[...] = jnp.zeros_like(part)
    terms[...] = jnp.zeros_like(terms)
    gsum[...] = jnp.zeros_like(gsum)
    spread[...] = jnp.zeros_like(spread)
    for load in loads:
        load.wait()
    pack(counts, jac, res, ids, tail, own4, own2, own8)
    pl.semaphore_wait(barrier, n + m - 2)

    def lanes_of(peer, first, count):
        return pl.ds(pl.multiple_of(peer * cap + first, 128), count)

    def handing(i, kinds):
        peer = flip(i)
        low, high = lanes_of(peer, 0, cut), lanes_of(peer, cut, cap - cut)
        sent = (
            own2.at[:, lanes_of(peer, 0, cap)], jac.at[0:16, low], own4.at[:, low], own8.at[:, high],
            jac.at[0:16, high], tail.at[:, high],
        )
        taken = (got2.at[i], got16.at[i], got4.at[i], got8.at[i], late16.at[i], late2.at[i])
        return [
            pltpu.make_async_remote_copy(
                src_ref=sent[k], dst_ref=taken[k], send_sem=x_send.at[k, i], recv_sem=x_recv.at[k, i],
                device_id={"obs": peer}, device_id_type=MESH,
            )
            for k in kinds
        ]

    def start(kinds, first, last):
        def one(i):
            for copy in handing(first + last - 1 - i, kinds):
                copy.start()

        each(first, last, one)

    start((0,), 1, n)
    start((1, 2, 3), 2, n)
    start((1, 2, 3, 4, 5), 1, 2)
    early = ready.shape[0] == n
    side = lax.rem(rep, PAIR)

    def hot_at(i):
        return hots.at[i if early else 0]

    def prepare(o, carry):
        ready[o] = one_hot_of(lax.rem(side_ids(o, side, half, cmap, width), LOW), LOW)
        return carry

    def see(i):
        hot_at(i)[...] = one_hot_of(place_of(got2[i, 0:1], width)[1], width)

    def foresee(i, carry):
        for copy in handing(i, (0,)):
            copy.wait_recv()
        if early:
            see(i)
        return carry

    def gradient_of(i):
        most, four = got16[i], got4[i]
        trail = jnp.concatenate([most[9:16], four[0:2]], axis=0)
        near = most[0:9] * four[2:3] + trail * four[3:4]
        eight = jnp.concatenate([near[0:8], got8[i]], axis=1)
        ninth = jnp.concatenate([near[8:9], got2[i, 1:2, cut:]], axis=1)
        add_gradient(eight, jnp.concatenate([got2[i, 0:1], ninth], axis=0), hot_at(i)[...], gsum, m)

    def low_block(i):
        if not early:
            see(i)
        add_block(got16[i], got4[i, 0:2], got2[i, 0:1, 0:cut], hot_at(i)[:, 0:cut], terms.at[:, 0:cut], part)

    def take(i, carry):
        for copy in handing(i, (1, 2, 3)):
            copy.wait_recv()
        if not early:
            see(i)
        gradient_of(i)
        return carry

    def take_both(i, carry):
        take(i, carry)
        low_block(i)
        return carry

    def take_low(i, carry):
        low_block(i)
        return carry

    def take_late(i, carry):
        for copy in handing(i, (4, 5)):
            copy.wait_recv()
        if not early:
            see(i)
        add_block(late16[i], late2[i], got2[i, 0:1, cut:], hot_at(i)[:, cut:], terms.at[:, 0 : cap - cut], part)
        return carry

    mylanes = lanes_of(me, 0, cap)
    hot_at(0)[...] = one_hot_of(place_of(own2[0:1, mylanes], width)[1], width)
    add_gradient(own8[:, mylanes], own2[:, mylanes], hot_at(0)[...], gsum, m)
    add_block(jac[0:16, mylanes], tail[:, mylanes], own2[0:1, mylanes], hot_at(0)[...], terms, part)
    lax.fori_loop(1, n, foresee, 0)
    if early:
        lax.fori_loop(0, n, prepare, 0)
    inline = min(INLINE, n)
    lax.fori_loop(1, inline, take_both, 0)
    lax.fori_loop(inline, n, take, 0)
    for h in range(m):
        eight = gsum[h * 16 : h * 16 + 8, :] + gsum[h * 16 + 8 : h * 16 + 16, :]
        ninth = m * 16 + h
        for k in range(8):
            piece[h, k] = eight[k : k + 1]
        piece[h, 8] = gsum[ninth : ninth + 1, :] + gsum[ninth + m : ninth + m + 1, :]

    def to_rep(src, dst, s, r, peer):
        return pltpu.make_async_remote_copy(
            src_ref=src, dst_ref=dst, send_sem=s, recv_sem=r, device_id={"rep": peer}, device_id_type=MESH
        )

    heads = []
    for i in range(1, m):
        peer = lax.rem(rep + i, m)
        heads.append(to_rep(piece.at[peer], land.at[i], a_send.at[i], a_recv.at[i], peer))
    for copy in heads:
        copy.start()
    start((4, 5), 2, n)
    lax.fori_loop(inline, n, take_low, 0)
    lax.fori_loop(1, min(EARLY, n), take_late, 0)
    for copy in heads:
        copy.wait_recv()
    summed = piece[rep]
    for i in range(1, m):
        summed = summed + land[i]
    mine[...] = summed
    grads[lax.div(rep, PAIR), me] = summed

    def reach(i, j):
        where = {"obs": flip(i), "rep": lax.rem(rep + PAIR * j, m)}
        return [
            pltpu.make_async_remote_copy(
                src_ref=mine, dst_ref=grads.at[lax.div(rep, PAIR), me], send_sem=g_send.at[i, j],
                recv_sem=g_recv.at[i, j], device_id=where, device_id_type=MESH,
            )
        ]

    def spread_out(i):
        for j in reversed(range(half)):
            for copy in reach(i, j):
                copy.start()

    each(1, n, spread_out)
    for j in range(1, half):
        for copy in reach(0, j):
            copy.start()

    def place(i, first):
        source = flip(i)
        for j in range(first, half):
            for copy in reach(i, j):
                copy.wait_recv()
        rows = [jnp.concatenate([grads[j, source, k] for j in range(half)], axis=1) for k in range(9)]
        eight, ninth = jnp.concatenate(rows[0:8], axis=0), rows[8]
        here = side_ids(source, side, half, cmap, width)
        place_chunk(eight, ninth, here, ready[source] if early else None, spread)

    def settle(i, carry):
        place(i, 0)
        return carry

    lax.fori_loop(min(EARLY, n), n, take_late, 0)
    mine_at, other_at = side * half, (1 - side) * half
    folds, wide, back = [], [], []
    for h in range(half):
        folds.append(to_rep(part.at[other_at + h], fold.at[h], b_send.at[h], b_recv.at[h], sibling))
        for j in range(1, half):
            peer = lax.rem(rep + PAIR * j, m)
            wide.append(to_rep(total.at[h], landed.at[j, h], w_send.at[j, h], w_recv.at[j, h], peer))
        back.append(to_rep(blocks.at[mine_at + h], blocks.at[mine_at + h], d_send.at[h], d_recv.at[h], sibling))
    for copy in folds:
        copy.start()
    for h in range(half):
        folds[h].wait_recv()
        total[h] = part[mine_at + h] + fold[h]
        for copy in wide[h * (half - 1) : (h + 1) * (half - 1)]:
            copy.start()
    def drain(i):
        for copy in handing(i, (0, 1, 2, 3, 4, 5)):
            copy.wait_send()

    def drain_reach(i):
        for j in range(half):
            for copy in reach(i, j):
                copy.wait_send()

    each(1, n, drain)
    for copy in heads + folds:
        copy.wait_send()
    place(0, 1)
    lax.fori_loop(1, n, settle, 0)
    swaps = []
    highs, step = gradient.shape[1] // LOW, gradient.shape[1] // CUTS
    for c in range(CUTS):
        lanes = pl.ds(c * step, step)
        lay_out(spread, out8, out9, c * highs // CUTS, (c + 1) * highs // CUTS)
        swaps.append(to_rep(out8.at[:, lanes], sib8.at[:, lanes], c_send.at[0, c], c_recv.at[0, c], sibling))
        swaps.append(to_rep(out9.at[:, lanes], sib9.at[:, lanes], c_send.at[1, c], c_recv.at[1, c], sibling))
        for copy in swaps[-2:]:
            copy.start()
    each(1, n, drain_reach)
    for j in range(1, half):
        for copy in reach(0, j):
            copy.wait_send()
    for h in range(half):
        for copy in wide[h * (half - 1) : (h + 1) * (half - 1)]:
            copy.wait_recv()
        full = total[h]
        for j in range(1, half):
            full = full + landed[j, h]
        blocks[mine_at + h] = full
        back[h].start()
    for copy in wide:
        copy.wait_send()
    for c in range(CUTS):
        lanes = slice(c * step, (c + 1) * step)
        for copy in swaps[2 * c : 2 * c + 2]:
            copy.wait_recv()
        gradient[0:8, lanes] = out8[:, lanes] + sib8[:, lanes]
        gradient[8:9, lanes] = out9[:, lanes] + sib9[:, lanes]
    for copy in back:
        copy.wait_recv()
    expand(blocks, out)

    for copy in back + swaps:
        copy.wait_send()


def write_kernel(gradient, blocks, gradient_out, blocks_out, out_sem):
    def cut(ref, count):
        step = ref.shape[1] // count
        return [ref.at[:, pl.ds(c * step, step)] for c in range(count)]

    jobs = list(zip(cut(blocks, 2), cut(blocks_out, 2)))
    jobs += list(zip(cut(gradient, 4), cut(gradient_out, 4)))
    writes = [pltpu.make_async_copy(job[0], job[1], out_sem.at[j]) for j, job in enumerate(jobs)]
    for write in writes:
        write.start()
    for write in writes:
        write.wait()


def local(jacobians, residuals, camera_local, bucket_counts, camera_map):
    n, m = lax.axis_size("obs"), lax.axis_size("rep")
    slots = jacobians.shape[1]
    cap = slots // n
    cut = cap // 2
    cams = camera_map.shape[0]
    width = CAM_DEV // m
    highs = cams // LOW
    half = m // PAIR
    dma = pltpu.SemaphoreType.DMA
    early = n * LOW * CAM_DEV * 2 <= 8 * MIB
    kept = n if early else 1
    held = 16 * cams * 4 + 88 * CAM_DEV * 4
    limit = 60 * MIB - max(0, held - 2 * MIB)
    gradient, out = pl.pallas_call(
        functools.partial(main_kernel, n, m),
        out_shape=(VMEM((9, cams), F32), VMEM((81, CAM_DEV), F32)),
        in_specs=[pl.BlockSpec(memory_space=pltpu.SMEM)] + [pl.BlockSpec(memory_space=pltpu.HBM)] * 4,
        out_specs=(vspec(), vspec()),
        scratch_shapes=[
            VMEM((18, slots), F32),
            VMEM((2, slots), F32),
            VMEM((1, slots), jnp.int32),
            VMEM((1, cams), jnp.int32),
            dma((4,)),
            VMEM((2, slots), F32),
            VMEM((4, slots), F32),
            VMEM((2, slots), F32),
            VMEM((8, slots), F32),
            VMEM((n, 16, cut), F32),
            VMEM((n, 4, cut), F32),
            VMEM((n, 2, cap), F32),
            VMEM((n, 8, cap - cut), F32),
            VMEM((n, 16, cap - cut), F32),
            VMEM((n, 2, cap - cut), F32),
            VMEM((kept, width, cap), BF16),
            VMEM((KEPT, cap), F32),
            VMEM((m * 18, width), F32),
            VMEM((m, KEPT, width), F32),
            VMEM((half, KEPT, width), F32),
            VMEM((half, half, KEPT, width), F32),
            VMEM((half, KEPT, width), F32),
            VMEM((m, KEPT, width), F32),
            VMEM((m, 9, 1, width), F32),
            VMEM((m, 9, 1, width), F32),
            VMEM((9, 1, width), F32),
            VMEM((half, n, 9, 1, width), F32),
            VMEM((kept, LOW, half * width), BF16),
            VMEM((highs * 18, LOW), F32),
            VMEM((8, cams), F32),
            VMEM((1, cams), F32),
            VMEM((8, cams), F32),
            VMEM((1, cams), F32),
            dma((6, n)),
            dma((6, n)),
            dma((m,)),
            dma((m,)),
            dma((n, half)),
            dma((n, half)),
            dma((2, CUTS)),
            dma((2, CUTS)),
            dma((half,)),
            dma((half,)),
            dma((half, half)),
            dma((half, half)),
            dma((half,)),
            dma((half,)),
        ],
        compiler_params=pltpu.CompilerParams(collective_id=0, has_side_effects=True, vmem_limit_bytes=limit),
    )(bucket_counts, jacobians, residuals, camera_local.reshape(1, slots), camera_map.reshape(1, cams))
    anywhere = pl.BlockSpec(memory_space=pl.ANY)
    shapes = (jax.ShapeDtypeStruct(gradient.shape, F32), jax.ShapeDtypeStruct(out.shape, F32))
    return pl.pallas_call(
        write_kernel,
        out_shape=shapes,
        in_specs=[vspec()] * 2,
        out_specs=(anywhere, anywhere),
        scratch_shapes=[dma((6,))],
        compiler_params=pltpu.CompilerParams(vmem_limit_bytes=2 * MIB),
    )(gradient, out)


def solution(mesh):
    in_specs = (
        P(None, ("obs", "rep")),
        P(None, ("obs", "rep")),
        P(("obs", "rep")),
        P(("obs", "rep"), None),
        P(),
    )
    out_specs = (P(), P(None, "obs"))
    return jax.shard_map(local, mesh=mesh, in_specs=in_specs, out_specs=out_specs, check_vma=False)
```
